128 devices in a mesh: row: 8 (over z, y_hi), col: 16 (over x, y_lo, core).
Axes of the slice: x: 4, y: 4 (y_hi: 2, y_lo: 2; y = y_hi * 2 + y_lo), z: 4, core: 2. Of those that a mesh axis runs over, the one named last changes fastest.
Arguments:
- atom_y: float32 [65536], P('col'), may hold values from 0 to 1024, as said below
- atom_x: float32 [65536], P('col'), may hold values from 0 to 1024
- atom_weight: float32 [65536], P('col'), may hold values from 0.5 to 2
- beam_ky: int32 [128], replicated, may hold values from -16 to 16
- beam_kx: int32 [128], replicated, may hold values from -16 to 16
- beam_amplitude: float32 [128], replicated, may hold values from 0.2 to 1.8
- crop_offset: int32 [2], replicated, may hold values from 0 to 512
- probe_y: int32 [8, 16, 128], P('row', 'col'), may hold values from 0 to 511
- probe_x: int32 [8, 16, 128], P('row', 'col'), may hold values from 0 to 511
Outputs:
- intensity: float32 [8, 16, 128, 2048], P('row', 'col')
The draws below stay inside these ranges and needn't reach their ends.
Inputs may be any that keep to these rules, and one draw needn't show every extreme that they name: Rows are grouped in bands of 16; atom i of each atom block (counted from the block's first atom) lies in band i // 64, that is 16 * band <= atom_y < 16 * band + 16.
All inputs are finite; a program needn't handle non-finite values.
Results may differ from the reference program's by a relative error of at most 0.012.
Values may be sent and summed in bfloat16 or wider, within the bound.
A program may use at most 64 MiB of HBM per device.

```python
import math
import jax
import jax.numpy as jnp
from jax import lax

N = 1024
WIN = 512
ATOM_BLK = 4096
PROBES = 128
ATOMS = 65536
BEAMS = 128
N_ROW = 8
N_COL = 16


def draw_atom_y(key, part):
    band_total = N // 16
    per_band = ATOM_BLK // band_total
    position = jnp.arange(ATOMS, dtype=jnp.int32) % ATOM_BLK
    band_of = (position // per_band).astype(jnp.float32)
    inside = jax.random.uniform(jax.random.fold_in(key, 11), (ATOMS,), jnp.float32, 0.0, 16.0)
    return jnp.minimum(band_of * 16.0 + inside, band_of * 16.0 + 15.999)


def set_ends(drawn, rng, least, high):
    longest = drawn.shape.index(max(drawn.shape))
    spots = []
    for shift in (0, 1):
        where = [jax.random.randint(jax.random.fold_in(rng, axis), (), 0, length) for axis, length in enumerate(drawn.shape)]
        where[longest] = (where[longest] + shift) % drawn.shape[longest]
        spots.append(tuple(where))
    return drawn.at[spots[0]].set(least).at[spots[1]].set(high)


def block_scale(own_key, shape, split, smallest, high):
    factor_of = 1.0
    for axis_at, shards_of in split:
        heights = jax.random.uniform(jax.random.fold_in(jax.random.fold_in(own_key, 6), axis_at), (shards_of,), jnp.float32, smallest / len(split), high / len(split))
        factor_of = factor_of * jnp.repeat(jnp.exp(heights), shape[axis_at] // shards_of).reshape((-1,) + (1,) * (len(shape) - 1 - axis_at))
    return factor_of


def setup_inputs(seed: int = 0) -> dict:
    key_of = jax.random.split(jax.random.key(seed), 10)
    atom_y = draw_atom_y(jax.random.fold_in(key_of[9], 71), 0)
    atom_x = jnp.clip(1024.0 * jax.random.uniform(key_of[1], (ATOMS,), jnp.float32) ** block_scale(key_of[1], (ATOMS,), ((0, 16),), -0.2, 0.2), 0.0, 1024.0)
    atom_weight = jnp.clip(0.5 + 1.5 * jax.random.uniform(key_of[2], (ATOMS,), jnp.float32) ** block_scale(key_of[2], (ATOMS,), ((0, 16),), -0.2, 0.2), 0.5, 2.0)
    beam_ky = set_ends(jax.random.randint(key_of[3], (BEAMS,), 0 - N // 64, N // 64 + 1), jax.random.fold_in(key_of[3], 1), 0 - N // 64, (N // 64 + 1) - 1).astype(jnp.int32)
    beam_kx = set_ends(jax.random.randint(key_of[4], (BEAMS,), 0 - N // 64, N // 64 + 1), jax.random.fold_in(key_of[4], 1), 0 - N // 64, (N // 64 + 1) - 1).astype(jnp.int32)
    beam_amplitude = jnp.clip(jax.random.uniform(key_of[5], (BEAMS,), jnp.float32, 0.2, 1.8), 0.2, 1.8)
    crop_offset = jax.random.randint(key_of[6], (2,), 0, N - WIN + 1).astype(jnp.int32)
    probe_y = set_ends(jax.random.randint(key_of[7], (N_ROW, N_COL, PROBES), 0, WIN), jax.random.fold_in(key_of[7], 1), 0, WIN - 1).astype(jnp.int32)
    probe_x = set_ends(jax.random.randint(key_of[8], (N_ROW, N_COL, PROBES), 0, WIN), jax.random.fold_in(key_of[8], 1), 0, WIN - 1).astype(jnp.int32)
    return dict(atom_y=atom_y, atom_x=atom_x, atom_weight=atom_weight, beam_ky=beam_ky, beam_kx=beam_kx, beam_amplitude=beam_amplitude, crop_offset=crop_offset, probe_y=probe_y, probe_x=probe_x)


interaction = 1.0
gauss_width = 2.0
two_pi = 2.0 * math.pi

def unit_phase(integer_phase, modulus, factor):
    angle = two_pi / modulus * jnp.mod(integer_phase, modulus).astype(jnp.float32)
    return (jnp.cos(angle) * factor, jnp.sin(angle) * factor)

def complex_dot(left_re, left_im, right_re, right_im):
    real = jnp.dot(left_re, right_re, preferred_element_type=jnp.float32) - jnp.dot(left_im, right_im, preferred_element_type=jnp.float32)
    imag = jnp.dot(left_re, right_im, preferred_element_type=jnp.float32) + jnp.dot(left_im, right_re, preferred_element_type=jnp.float32)
    return (real, imag)

def gaussians(centres, count):
    places = jnp.arange(count).astype(jnp.float32)
    return jnp.exp(-jnp.square((places[None, :] - centres[:, None]) / gauss_width))

def reference(atom_y, atom_x, atom_weight, beam_ky, beam_kx, beam_amplitude, crop_offset, probe_y, probe_x):
    profile_y = gaussians(atom_y, N)
    profile_x = gaussians(atom_x, N) * atom_weight[:, None]
    potential = lax.dot_general(profile_y, profile_x, (((0,), (0,)), ((), ())), precision=lax.Precision.HIGHEST, preferred_element_type=jnp.float32)
    index = jnp.arange(N, dtype=jnp.int32)
    forward_re, forward_im = unit_phase(-index[:, None] * index[None, :], N, 1.0)
    forward_re = forward_re.astype(jnp.bfloat16)
    forward_im = forward_im.astype(jnp.bfloat16)
    signed = jnp.where(index < N // 2, index, index - N)
    square = signed * signed
    prop_re, prop_im = unit_phase(-(square[:, None] + square[None, :]), 4 * N, 1.0)
    window = jnp.arange(WIN, dtype=jnp.int32)
    back_yre, back_yim = unit_phase((crop_offset[0] + window)[:, None] * index[None, :], N, 1.0 / N)
    back_yre = back_yre.astype(jnp.bfloat16)
    back_yim = back_yim.astype(jnp.bfloat16)
    back_xre, back_xim = unit_phase(index[:, None] * (crop_offset[1] + window)[None, :], N, 1.0 / N)
    back_xre = back_xre.astype(jnp.bfloat16)
    back_xim = back_xim.astype(jnp.bfloat16)

    def one_beam(beam_index):
        beam_phase = jnp.mod(beam_ky[beam_index] * index[:, None] + beam_kx[beam_index] * index[None, :], N)
        angle = interaction * potential + two_pi / N * beam_phase.astype(jnp.float32)
        wave_re = jnp.cos(angle).astype(jnp.bfloat16)
        wave_im = jnp.sin(angle).astype(jnp.bfloat16)
        first_re, first_im = complex_dot(forward_re, forward_im, wave_re, wave_im)
        first_re = first_re.astype(jnp.bfloat16)
        first_im = first_im.astype(jnp.bfloat16)
        second_re, second_im = complex_dot(first_re, first_im, forward_re, forward_im)
        moved_re = (second_re * prop_re - second_im * prop_im).astype(jnp.bfloat16)
        moved_im = (second_re * prop_im + second_im * prop_re).astype(jnp.bfloat16)
        third_re, third_im = complex_dot(back_yre, back_yim, moved_re, moved_im)
        third_re = third_re.astype(jnp.bfloat16)
        third_im = third_im.astype(jnp.bfloat16)
        final_re, final_im = complex_dot(third_re, third_im, back_xre, back_xim)
        return jnp.stack([final_re.astype(jnp.bfloat16), final_im.astype(jnp.bfloat16)])
    waves = lax.map(one_beam, jnp.arange(BEAMS, dtype=jnp.int32))
    tile_rows = WIN // N_ROW
    tile_cols = WIN // N_COL
    tiles = waves.reshape(BEAMS, 2, N_ROW, tile_rows, N_COL, tile_cols).transpose(2, 4, 1, 0, 3, 5)
    tiles = tiles.reshape(N_ROW * N_COL, 2, BEAMS, tile_rows * tile_cols)
    weights = beam_amplitude / math.sqrt(BEAMS)

    def one_tile(operands):
        tile, where_y, where_x = operands
        integer = beam_ky[None, :] * (where_y[:, None] + crop_offset[0]) + beam_kx[None, :] * (where_x[:, None] + crop_offset[1])
        coeff_re, coeff_im = unit_phase(-integer, N, 1.0)
        coeff_re = (coeff_re * weights[None, :]).astype(jnp.bfloat16)
        coeff_im = (coeff_im * weights[None, :]).astype(jnp.bfloat16)
        probe_re, probe_im = complex_dot(coeff_re, coeff_im, tile[0], tile[1])
        return jnp.square(probe_re) + jnp.square(probe_im)
    result = lax.map(one_tile, (tiles, probe_y.reshape(N_ROW * N_COL, PROBES), probe_x.reshape(N_ROW * N_COL, PROBES)))
    return result.reshape(N_ROW, N_COL, PROBES, tile_rows * tile_cols)
```

```python
import functools
import math

import jax
import jax.numpy as jnp
import numpy as np
from jax import lax
from jax.experimental import pallas as pl
from jax.experimental.pallas import tpu as pltpu
from jax.sharding import PartitionSpec as P

N = 1024
WIN = 512
ROWS = 8
COLS = 16
TILT = 16
KINDS = 2 * TILT + 1
TILE_Y = WIN // ROWS
TILE_X = WIN // COLS
BAND_ROWS = N // ROWS
GROUPS = 7
MESH = pl.DeviceIdType.MESH


EDGE = np.concatenate([np.arange(N // 2 - TILT, N // 2), np.arange(-N // 2, -N // 2 + TILT)])


def turn(number, modulus):
    return np.exp(2j * np.pi * np.mod(number, modulus) / modulus)


def fresnel():
    freq = np.arange(-N // 2, N // 2)
    half = np.arange(2 * N)
    return (turn(np.outer(half, freq), 2 * N) * turn(-freq * freq, 4 * N)[None, :]).sum(1) / N


def basis(length):
    table = fresnel()
    place = np.arange(N)
    shift = np.arange(length + TILT)
    apart = 2 * (shift[:, None] - TILT // 2 - place[None, :])
    edge = turn(-EDGE * EDGE, 4 * N)[:, None] * turn(-np.outer(EDGE, place), N) / N
    return np.concatenate([table[np.mod(apart, 2 * N)], table[np.mod(apart + 1, 2 * N)], edge])


def synthesis(length):
    count = length + TILT
    pixel = np.arange(length)
    out = np.zeros((KINDS, length, 2 * count + 2 * TILT), complex)
    for kind in range(KINDS):
        tilt = kind - TILT
        phase = turn(tilt * pixel, N)
        if tilt % 2 == 0:
            place = pixel - tilt // 2 + TILT // 2
        else:
            place = count + pixel - (tilt + 1) // 2 + TILT // 2
        out[kind, pixel, place] = phase
        moved = EDGE + tilt
        flips = ((moved < -N // 2) | (moved >= N // 2)) & (moved % 2 != 0)
        wrapped = -2 * turn((2 * pixel[:, None] - tilt) * EDGE[None, :], 2 * N)
        out[kind, :, 2 * count :] = phase[:, None] * np.where(flips[None, :], wrapped, 0)
    return out


@functools.lru_cache(None)
def tables():
    across = basis(TILE_X).T
    across = np.concatenate([across.real, across.imag], 1)
    across = np.concatenate([across, across], 0)
    down = basis(TILE_Y)
    down = np.concatenate([down.real, down.imag], 0)
    spread_y = synthesis(TILE_Y)
    order = (4 * np.arange(TILE_Y // 4)[None, :] + np.arange(4)[:, None]).reshape(-1)
    spread_y = spread_y[:, order]
    spread_y = np.concatenate([spread_y.real, spread_y.imag], 2).reshape(KINDS * TILE_Y, -1)
    spread_x = synthesis(TILE_X).transpose(0, 2, 1)
    top = np.concatenate([spread_x.real, spread_x.imag], 2)
    bottom = np.concatenate([-spread_x.imag, spread_x.real], 2)
    spread_x = np.concatenate([top, bottom], 1)
    spread_x = np.concatenate([spread_x, spread_x], 2)
    return tuple(
        value.astype(jnp.bfloat16) for value in (across, down, spread_y, spread_x)
    )


@functools.lru_cache(None)
def wave_fit():
    grid = np.cos(np.pi * (np.arange(4000) + 0.5) / 4000) * np.pi
    square = grid * grid
    powers = (square / np.pi**2)[:, None] ** np.arange(8)[None, :]
    even = np.linalg.lstsq(powers, np.cos(grid), rcond=None)[0] / np.pi ** (2 * np.arange(8))
    odd = np.linalg.lstsq(powers, np.sin(grid) / grid, rcond=None)[0] / np.pi ** (2 * np.arange(8))
    return [float(v) for v in even], [float(v) for v in odd]


def cos_sin_reduced(angle):
    even, odd = wave_fit()
    square = angle * angle
    cosine = jnp.full_like(angle, even[-1])
    sine = jnp.full_like(angle, odd[-1])
    for e, o in zip(even[-2::-1], odd[-2::-1]):
        cosine = cosine * square + e
        sine = sine * square + o
    return cosine, sine * angle


TURN_A = 6.28125
TURN_B = 0.0019350051879882812
TURN_C = 2.0 * math.pi - TURN_A - TURN_B


def cos_sin(angle):
    whole = jnp.floor(angle * (0.5 / math.pi) + 0.5)
    return cos_sin_reduced(((angle - whole * TURN_A) - whole * TURN_B) - whole * TURN_C)


def potential_kernel(
    crop,
    atom_y,
    atom_x,
    atom_weight,
    across_hbm,
    down_hbm,
    out,
    prof_x,
    prof_y,
    part,
    landed,
    whole,
    wave,
    across,
    down,
    moved,
    gathered,
    table_sem,
    part_send,
    part_recv,
    whole_send,
    whole_recv,
    moved_send,
    moved_recv,
):
    row = lax.axis_index("row")
    col = lax.axis_index("col")
    barrier = pltpu.get_barrier_semaphore()
    for step in range(1, COLS):
        peer = lax.rem(col + step, COLS)
        pl.semaphore_signal(barrier, inc=1, device_id={"col": peer}, device_id_type=MESH)
    for step in range(1, ROWS):
        peer = lax.rem(row + step, ROWS)
        pl.semaphore_signal(barrier, inc=1, device_id={"row": peer}, device_id_type=MESH)
    start = pl.multiple_of(N - TILE_X * col, TILE_X)
    across_copy = pltpu.make_async_copy(
        across_hbm.at[pl.ds(start, N)], across, table_sem.at[0]
    )
    down_copy = pltpu.make_async_copy(down_hbm, down, table_sem.at[1])
    across_copy.start()
    down_copy.start()

    crop_y = crop[0]
    crop_x = crop[1]
    first_y = (BAND_ROWS * row + crop_y) & (N - 1)
    first_group = ((first_y + (N - 21)) & (N - 1)) // 32
    at_y = ((lax.broadcasted_iota(jnp.int32, (BAND_ROWS, 128), 0) + first_y) & (N - 1)).astype(
        jnp.float32
    )
    lane = lax.broadcasted_iota(jnp.int32, (128, N), 1)
    at_x = ((lane + crop_x) & (N - 1)).astype(jnp.float32)
    for group in range(GROUPS):
        index = (first_group + group) & 31
        here_y = atom_y[pl.ds(index, 1), :]
        here_x = atom_x[pl.ds(index, 1), :]
        here_w = atom_weight[pl.ds(index, 1), :]
        apart = (at_y - here_y) * 0.5
        value = jnp.exp(-(apart * apart)) * here_w
        prof_y[:, 128 * group : 128 * group + 128] = value.astype(jnp.bfloat16)
        column = jnp.transpose(jnp.broadcast_to(here_x, (128, 128)))
        column = jnp.concatenate([column] * (N // 128), axis=1)
        apart = (at_x - column) * 0.5
        prof_x[128 * group : 128 * group + 128, :] = jnp.exp(-(apart * apart)).astype(jnp.bfloat16)
    partial = jnp.dot(prof_y[...], prof_x[...], preferred_element_type=jnp.float32)
    for block in range(COLS):
        high, side = block // 2, block % 2
        part[block] = partial[16 * high : 16 * high + 16, 512 * side : 512 * side + 512].astype(
            jnp.bfloat16
        )
    pl.semaphore_wait(barrier, COLS - 1 + ROWS - 1)

    copies = []
    for step in range(1, COLS):
        peer = lax.rem(col + step, COLS)
        copy = pltpu.make_async_remote_copy(
            src_ref=part.at[peer],
            dst_ref=landed.at[step],
            send_sem=part_send.at[step],
            recv_sem=part_recv.at[step],
            device_id={"col": peer},
            device_id_type=MESH,
        )
        copy.start()
        copies.append(copy)
    total = part[col].astype(jnp.float32)
    for step in range(1, COLS):
        copies[step - 1].wait_recv()
        total = total + landed[step].astype(jnp.float32)
    whole[col] = total.astype(jnp.bfloat16)

    shares = []
    for step in range(1, COLS):
        peer = lax.rem(col + step, COLS)
        share = pltpu.make_async_remote_copy(
            src_ref=whole.at[col],
            dst_ref=whole.at[col],
            send_sem=whole_send.at[step],
            recv_sem=whole_recv.at[step],
            device_id={"col": peer},
            device_id_type=MESH,
        )
        share.start()
        shares.append(share)
    for share in shares:
        share.wait_recv()
    for block in range(COLS):
        high, side = block // 2, block % 2
        real, imag = cos_sin(whole[block].astype(jnp.float32))
        wave[16 * high : 16 * high + 16, 512 * side : 512 * side + 512] = real.astype(jnp.bfloat16)
        wave[
            BAND_ROWS + 16 * high : BAND_ROWS + 16 * high + 16, 512 * side : 512 * side + 512
        ] = imag.astype(jnp.bfloat16)

    across_copy.wait()
    product = jnp.dot(wave[...], across[...], preferred_element_type=jnp.float32)
    real = product[:128, :128] - product[128:, 128:]
    imag = product[:128, 128:] + product[128:, :128]
    both = jnp.concatenate([real, imag], axis=1).astype(jnp.bfloat16)
    moved[0] = both[:64]
    moved[1] = both[64:]
    hops = []
    for step in range(1, ROWS):
        peer = lax.rem(row + step, ROWS)
        for half in range(2):
            hop = pltpu.make_async_remote_copy(
                src_ref=moved.at[half],
                dst_ref=gathered.at[(2 * row + half - peer + 16) & 15],
                send_sem=moved_send.at[2 * step + half],
                recv_sem=moved_recv.at[2 * step + half],
                device_id={"row": peer},
                device_id_type=MESH,
            )
            hop.start()
            hops.append(hop)
    gathered[row] = both[:64]
    gathered[(row + 1) & 15] = both[64:]
    down_copy.wait()
    for hop in hops:
        hop.wait_recv()

    product = jnp.dot(
        down[...], gathered[...].reshape(N, 256), preferred_element_type=jnp.float32
    )
    deep = product.shape[0] // 2
    real = (product[:deep, :128] - product[deep:, 128:]).astype(jnp.bfloat16)
    imag = (product[:deep, 128:] + product[deep:, :128]).astype(jnp.bfloat16)
    out[:deep, :128] = real
    out[:deep, 128:] = imag
    out[deep:, :128] = -imag
    out[deep:, 128:] = real
    for copy in copies + shares + hops:
        copy.wait_send()


def probe_kernel(
    beam_y,
    beam_x,
    core,
    spread_y,
    spread_x,
    tilt_y,
    tilt_x,
    amplitude,
    probe_y,
    probe_x,
    out,
    half,
    field_re,
    field_im,
):
    row = lax.axis_index("row")
    col = lax.axis_index("col")

    middle = core[...]

    def tilts(step, carry):
        rows = pl.ds(pl.multiple_of(step * 192, 192), 192)
        half[rows, :] = jnp.dot(
            spread_y[rows, :], middle, preferred_element_type=jnp.float32
        ).astype(jnp.bfloat16)
        return carry

    lax.fori_loop(0, KINDS * TILE_Y // 192, tilts, 0)

    group = lax.broadcasted_iota(jnp.int32, (16, 128), 1) // 32
    even = (group & 1) == 0

    def one_beam(beam):
        rows = pl.ds(pl.multiple_of((beam_y[beam] + TILT) * TILE_Y, TILE_Y), TILE_Y)
        value = jnp.dot(
            half[rows, :], spread_x[beam_x[beam] + TILT], preferred_element_type=jnp.float32
        )
        a, b, c, d = (value[16 * i : 16 * i + 16] for i in range(4))
        straight = jnp.where(
            group < 2, jnp.where(group == 0, a, b), jnp.where(group == 2, c, d)
        )
        crossed = jnp.where(
            group < 2, jnp.where(group == 0, b, a), jnp.where(group == 2, d, c)
        )
        crossed = jnp.where(even, pltpu.roll(crossed, 96, 1), pltpu.roll(crossed, 32, 1))
        rows = pl.ds(pl.multiple_of(beam * 16, 16), 16)
        field_re[rows, :] = jnp.where(even, straight, crossed)
        field_im[rows, :] = jnp.where(even, crossed, straight)

    def beams(step, carry):
        for inner in range(8):
            one_beam(step * 8 + inner)
        return carry

    lax.fori_loop(0, 16, beams, 0)

    ky = tilt_y[...]
    kx = tilt_x[...]
    at_y = jnp.transpose(jnp.broadcast_to(probe_y[...], (128, 128))) - TILE_Y * row
    at_x = jnp.transpose(jnp.broadcast_to(probe_x[...], (128, 128))) - TILE_X * col
    number = (4 * (ky * at_y + kx * at_x) + ky * ky + kx * kx) & (4 * N - 1)
    number = jnp.where(number >= 2 * N, number - 4 * N, number)
    real, imag = cos_sin_reduced(number.astype(jnp.float32) * (-2.0 * math.pi / (4 * N)))
    weight = amplitude[...] * (1.0 / math.sqrt(128.0))
    coefficient = jnp.concatenate([real * weight, imag * weight], axis=0).astype(jnp.bfloat16)
    for piece in range(16):
        rows = pl.ds(piece, 128, stride=16)
        field = jnp.concatenate([field_re[rows, :], field_im[rows, :]], axis=1)
        field = field.astype(jnp.bfloat16)
        product = jnp.dot(coefficient, field, preferred_element_type=jnp.float32)
        real = product[:128, :128] - product[128:, 128:]
        imag = product[:128, 128:] + product[128:, :128]
        out[:, 128 * piece : 128 * piece + 128] = real * real + imag * imag


def body(
    atom_y, atom_x, atom_weight, beam_ky, beam_kx, beam_amplitude, crop_offset, probe_y, probe_x
):
    across, down, spread_y, spread_x = (jnp.asarray(v) for v in tables())
    vmem = pl.BlockSpec(memory_space=pltpu.VMEM)
    smem = pl.BlockSpec(memory_space=pltpu.SMEM)
    anywhere = pl.BlockSpec(memory_space=pl.ANY)
    bf16 = jnp.bfloat16
    core = pl.pallas_call(
        potential_kernel,
        name="potential_to_basis",
        out_shape=jax.ShapeDtypeStruct((384, 256), bf16),
        in_specs=[smem, vmem, vmem, vmem, anywhere, anywhere],
        out_specs=vmem,
        scratch_shapes=[
            pltpu.VMEM((128 * GROUPS, N), bf16),
            pltpu.VMEM((BAND_ROWS, 128 * GROUPS), bf16),
            pltpu.VMEM((COLS, 16, 512), bf16),
            pltpu.VMEM((COLS, 16, 512), bf16),
            pltpu.VMEM((COLS, 16, 512), bf16),
            pltpu.VMEM((2 * BAND_ROWS, N), bf16),
            pltpu.VMEM((N, 256), bf16),
            pltpu.VMEM((384, N), bf16),
            pltpu.VMEM((2, 64, 256), bf16),
            pltpu.VMEM((16, 64, 256), bf16),
            pltpu.SemaphoreType.DMA((2,)),
            pltpu.SemaphoreType.DMA((COLS,)),
            pltpu.SemaphoreType.DMA((COLS,)),
            pltpu.SemaphoreType.DMA((COLS,)),
            pltpu.SemaphoreType.DMA((COLS,)),
            pltpu.SemaphoreType.DMA((2 * ROWS,)),
            pltpu.SemaphoreType.DMA((2 * ROWS,)),
        ],
        compiler_params=pltpu.CompilerParams(
            collective_id=0, has_side_effects=True, vmem_limit_bytes=24 * 2**20
        ),
    )(
        crop_offset,
        atom_y.reshape(32, 128),
        atom_x.reshape(32, 128),
        atom_weight.reshape(32, 128),
        across,
        down,
    )
    result = pl.pallas_call(
        probe_kernel,
        name="basis_to_probes",
        out_shape=jax.ShapeDtypeStruct((128, 2048), jnp.float32),
        in_specs=[smem, smem] + [vmem] * 8,
        out_specs=vmem,
        scratch_shapes=[
            pltpu.VMEM((KINDS * TILE_Y, 256), bf16),
            pltpu.VMEM((128 * 16, 128), jnp.float32),
            pltpu.VMEM((128 * 16, 128), jnp.float32),
        ],
        compiler_params=pltpu.CompilerParams(vmem_limit_bytes=24 * 2**20),
    )(
        beam_ky,
        beam_kx,
        core,
        spread_y,
        spread_x,
        beam_ky.reshape(1, 128),
        beam_kx.reshape(1, 128),
        beam_amplitude.reshape(1, 128),
        probe_y.reshape(1, 128),
        probe_x.reshape(1, 128),
    )
    return result[None, None]


def solution(mesh):
    return jax.shard_map(
        body,
        mesh=mesh,
        in_specs=(
            P("col"),
            P("col"),
            P("col"),
            P(),
            P(),
            P(),
            P(),
            P("row", "col", None),
            P("row", "col", None),
        ),
        out_specs=P("row", "col", None, None),
        check_vma=False,
    )
```

```python
import functools
import math

import jax
import jax.numpy as jnp
import numpy as np
from jax import lax
from jax.experimental import pallas as pl
from jax.experimental.pallas import tpu as pltpu
from jax.sharding import PartitionSpec as P

N = 1024
WIN = 512
ROWS = 8
COLS = 16
TILT = 16
KINDS = 2 * TILT + 1
TILE_Y = WIN // ROWS
TILE_X = WIN // COLS
BAND_ROWS = N // ROWS
GROUPS = 7
CHUNKS = 4
CHUNK_ROWS = BAND_ROWS // CHUNKS
SLICE_HIGH = CHUNK_ROWS // 16
SLICE_WIDE = N * SLICE_HIGH // COLS
PIECE = min(CHUNK_ROWS, TILE_Y)
LEAD = TILE_X * (COLS - 1)
MESH = pl.DeviceIdType.MESH


EDGE = np.concatenate([np.arange(N // 2 - TILT, N // 2), np.arange(-N // 2, -N // 2 + TILT)])


def turn(number, modulus):
    return np.exp(2j * np.pi * np.mod(number, modulus) / modulus)


def fresnel():
    freq = np.arange(-N // 2, N // 2)
    half = np.arange(2 * N)
    return (turn(np.outer(half, freq), 2 * N) * turn(-freq * freq, 4 * N)[None, :]).sum(1) / N


def basis(length):
    table = fresnel()
    place = np.arange(N)
    shift = np.arange(length + TILT)
    apart = 2 * (shift[:, None] - TILT // 2 - place[None, :])
    edge = turn(-EDGE * EDGE, 4 * N)[:, None] * turn(-np.outer(EDGE, place), N) / N
    return np.concatenate([table[np.mod(apart, 2 * N)], table[np.mod(apart + 1, 2 * N)], edge])


def synthesis(length):
    count = length + TILT
    pixel = np.arange(length)
    out = np.zeros((KINDS, length, 2 * count + 2 * TILT), complex)
    for kind in range(KINDS):
        tilt = kind - TILT
        phase = turn(tilt * pixel, N)
        if tilt % 2 == 0:
            place = pixel - tilt // 2 + TILT // 2
        else:
            place = count + pixel - (tilt + 1) // 2 + TILT // 2
        out[kind, pixel, place] = phase
        moved = EDGE + tilt
        flips = ((moved < -N // 2) | (moved >= N // 2)) & (moved % 2 != 0)
        wrapped = -2 * turn((2 * pixel[:, None] - tilt) * EDGE[None, :], 2 * N)
        out[kind, :, 2 * count :] = phase[:, None] * np.where(flips[None, :], wrapped, 0)
    return out


def two_parts(value, axis):
    high = value.astype(jnp.bfloat16).astype(np.float64)
    return np.concatenate([high, value - high], axis)


@functools.lru_cache(None)
def tables():
    across = basis(TILE_X).T
    across = two_parts(np.concatenate([across.real, across.imag], 1), 1)
    across = np.concatenate([across[N - LEAD :], across], 0)
    down = basis(TILE_Y)
    down = two_parts(np.concatenate([down.real, down.imag], 0), 0)
    spread_y = synthesis(TILE_Y)
    order = (4 * np.arange(TILE_Y // 4)[None, :] + np.arange(4)[:, None]).reshape(-1)
    spread_y = spread_y[:, order]
    spread_y = np.concatenate([spread_y.real, spread_y.imag], 2).reshape(KINDS * TILE_Y, -1)
    spread_x = synthesis(TILE_X).transpose(0, 2, 1)
    top = np.concatenate([spread_x.real, spread_x.imag], 2)
    bottom = np.concatenate([-spread_x.imag, spread_x.real], 2)
    spread_x = np.concatenate([top, bottom], 1)
    spread_x = np.concatenate([spread_x, spread_x], 2)
    return tuple(
        value.astype(jnp.bfloat16) for value in (across, down, spread_y, spread_x)
    )


@functools.lru_cache(None)
def wave_fit():
    grid = np.cos(np.pi * (np.arange(4000) + 0.5) / 4000) * np.pi
    square = grid * grid
    powers = (square / np.pi**2)[:, None] ** np.arange(8)[None, :]
    even = np.linalg.lstsq(powers, np.cos(grid), rcond=None)[0] / np.pi ** (2 * np.arange(8))
    odd = np.linalg.lstsq(powers, np.sin(grid) / grid, rcond=None)[0] / np.pi ** (2 * np.arange(8))
    return [float(v) for v in even], [float(v) for v in odd]


def cos_sin_reduced(angle):
    even, odd = wave_fit()
    square = angle * angle
    cosine = jnp.full_like(angle, even[-1])
    sine = jnp.full_like(angle, odd[-1])
    for e, o in zip(even[-2::-1], odd[-2::-1]):
        cosine = cosine * square + e
        sine = sine * square + o
    return cosine, sine * angle


TURN_A = 6.28125
TURN_B = 0.0019350051879882812
TURN_C = 2.0 * math.pi - TURN_A - TURN_B


def cos_sin(angle):
    whole = jnp.floor(angle * (0.5 / math.pi) + 0.5)
    return cos_sin_reduced(((angle - whole * TURN_A) - whole * TURN_B) - whole * TURN_C)


def slice_place(block):
    high, side = block % SLICE_HIGH, block // SLICE_HIGH
    return (
        slice(16 * high, 16 * high + 16),
        slice(SLICE_WIDE * side, SLICE_WIDE * side + SLICE_WIDE),
    )


def potential_kernel(
    crop_hbm,
    atom_y_hbm,
    atom_x_hbm,
    atom_weight_hbm,
    tilt_y_hbm,
    tilt_x_hbm,
    amplitude_hbm,
    probe_y_hbm,
    probe_x_hbm,
    across_hbm,
    down_hbm,
    spread_y_hbm,
    spread_x_hbm,
    core,
    coefficient,
    spread_y,
    spread_x,
    crop,
    atoms,
    beams,
    amplitude,
    prof_x,
    prof_y,
    part,
    landed,
    whole,
    wave,
    across,
    down,
    moved,
    gathered,
    table_sem,
    part_send,
    part_recv,
    whole_send,
    whole_recv,
    moved_send,
    moved_recv,
):
    row = lax.axis_index("row")
    col = lax.axis_index("col")
    start = pl.multiple_of(LEAD - TILE_X * col, TILE_X)
    loads = [
        pltpu.make_async_copy(source, target, table_sem.at[place])
        for place, (source, target) in enumerate(
            (
                (crop_hbm, crop),
                (atom_y_hbm, atoms.at[0]),
                (atom_x_hbm, atoms.at[1]),
                (atom_weight_hbm, atoms.at[2]),
                (tilt_y_hbm, beams.at[0]),
                (tilt_x_hbm, beams.at[1]),
                (probe_y_hbm, beams.at[2]),
                (probe_x_hbm, beams.at[3]),
                (amplitude_hbm, amplitude),
                (across_hbm.at[pl.ds(start, N)], across),
                (down_hbm, down),
                (spread_y_hbm, spread_y),
                (spread_x_hbm, spread_x),
            )
        )
    ]
    for load in loads[:4]:
        load.start()
    barrier = pltpu.get_barrier_semaphore()
    for step in range(1, COLS):
        peer = lax.rem(col + step, COLS)
        pl.semaphore_signal(barrier, inc=1, device_id={"col": peer}, device_id_type=MESH)
    for step in range(1, ROWS):
        peer = lax.rem(row + step, ROWS)
        pl.semaphore_signal(barrier, inc=1, device_id={"row": peer}, device_id_type=MESH)
    for load in loads[4:]:
        load.start()
    for load in loads[:4]:
        load.wait()

    crop_y = crop[0]
    crop_x = crop[1]
    first_y = (BAND_ROWS * row + crop_y) & (N - 1)
    first_group = ((first_y + (N - 21)) & (N - 1)) // 32
    at_y = ((lax.broadcasted_iota(jnp.int32, (BAND_ROWS, 128), 0) + first_y) & (N - 1)).astype(
        jnp.float32
    )
    lane = lax.broadcasted_iota(jnp.int32, (128, N), 1)
    at_x = ((lane + crop_x) & (N - 1)).astype(jnp.float32)
    for group in range(GROUPS):
        index = (first_group + group) & 31
        here_y = atoms[0, pl.ds(index, 1), :]
        here_x = atoms[1, pl.ds(index, 1), :]
        here_w = atoms[2, pl.ds(index, 1), :]
        apart = (at_y - here_y) * 0.5
        value = jnp.exp(-(apart * apart)) * here_w
        prof_y[:, 128 * group : 128 * group + 128] = value.astype(jnp.bfloat16)
        column = jnp.transpose(jnp.broadcast_to(here_x, (128, 128)))
        column = jnp.concatenate([column] * (N // 128), axis=1)
        apart = (at_x - column) * 0.5
        prof_x[128 * group : 128 * group + 128, :] = jnp.exp(-(apart * apart)).astype(jnp.bfloat16)
    partial = jnp.dot(prof_y[...], prof_x[...], preferred_element_type=jnp.float32)
    for chunk in range(CHUNKS):
        rows = partial[CHUNK_ROWS * chunk : CHUNK_ROWS * chunk + CHUNK_ROWS].astype(jnp.bfloat16)
        for block in range(COLS):
            part[chunk, block] = rows[slice_place(block)]
    pl.semaphore_wait(barrier, COLS - 1 + ROWS - 1)

    copies = []
    for chunk in range(CHUNKS):
        for step in range(1, COLS):
            peer = lax.rem(col + step, COLS)
            copy = pltpu.make_async_remote_copy(
                src_ref=part.at[chunk, peer],
                dst_ref=landed.at[chunk, step],
                send_sem=part_send.at[chunk, step],
                recv_sem=part_recv.at[chunk, step],
                device_id={"col": peer},
                device_id_type=MESH,
            )
            copy.start()
            copies.append(copy)

    for load in loads[4:9]:
        load.wait()
    ky = beams[0]
    kx = beams[1]
    at_y = jnp.transpose(jnp.broadcast_to(beams[2], (128, 128))) - TILE_Y * row
    at_x = jnp.transpose(jnp.broadcast_to(beams[3], (128, 128))) - TILE_X * col
    number = (4 * (ky * at_y + kx * at_x) + ky * ky + kx * kx) & (4 * N - 1)
    number = jnp.where(number >= 2 * N, number - 4 * N, number)
    real, imag = cos_sin_reduced(number.astype(jnp.float32) * (-2.0 * math.pi / (4 * N)))
    weight = amplitude[...] * (1.0 / math.sqrt(128.0))
    coefficient[:128] = (real * weight).astype(jnp.bfloat16)
    coefficient[128:] = (imag * weight).astype(jnp.bfloat16)

    shares = []
    for chunk in range(CHUNKS):
        total = part[chunk, col].astype(jnp.float32)
        for step in range(1, COLS):
            copies[(COLS - 1) * chunk + step - 1].wait_recv()
            total = total + landed[chunk, step].astype(jnp.float32)
        whole[chunk, col] = (total - 1.0).astype(jnp.bfloat16)
        for step in range(1, COLS):
            peer = lax.rem(col + step, COLS)
            share = pltpu.make_async_remote_copy(
                src_ref=whole.at[chunk, col],
                dst_ref=whole.at[chunk, col],
                send_sem=whole_send.at[chunk, step],
                recv_sem=whole_recv.at[chunk, step],
                device_id={"col": peer},
                device_id_type=MESH,
            )
            share.start()
            shares.append(share)

    loads[9].wait()
    hops = []
    for chunk in range(CHUNKS):
        for share in shares[(COLS - 1) * chunk : (COLS - 1) * (chunk + 1)]:
            share.wait_recv()
        for block in range(COLS):
            rows, columns = slice_place(block)
            real, imag = cos_sin(whole[chunk, block].astype(jnp.float32) + 1.0)
            wave[rows, columns] = real.astype(jnp.bfloat16)
            wave[slice(CHUNK_ROWS + rows.start, CHUNK_ROWS + rows.stop), columns] = imag.astype(
                jnp.bfloat16
            )
        product = jnp.dot(wave[...], across[...], preferred_element_type=jnp.float32)
        product = product[:, :256] + product[:, 256:]
        real = product[:CHUNK_ROWS, :128] - product[CHUNK_ROWS:, 128:]
        imag = product[:CHUNK_ROWS, 128:] + product[CHUNK_ROWS:, :128]
        both = jnp.concatenate([real, imag], axis=1).astype(jnp.bfloat16)
        pieces = CHUNK_ROWS // PIECE
        for piece in range(pieces):
            number = pieces * chunk + piece
            moved[number] = both[PIECE * piece : PIECE * piece + PIECE]
            for step in range(1, ROWS):
                peer = lax.rem(row + step, ROWS)
                place = row * (BAND_ROWS // PIECE) + number - peer * (TILE_Y // PIECE)
                hop = pltpu.make_async_remote_copy(
                    src_ref=moved.at[number],
                    dst_ref=gathered.at[(place + N) & (N // PIECE - 1)],
                    send_sem=moved_send.at[number, step],
                    recv_sem=moved_recv.at[number, step],
                    device_id={"row": peer},
                    device_id_type=MESH,
                )
                hop.start()
                hops.append(hop)
            place = row * ((BAND_ROWS - TILE_Y) // PIECE) + number
            gathered[place & (N // PIECE - 1)] = both[PIECE * piece : PIECE * piece + PIECE]
    loads[10].wait()
    for hop in hops:
        hop.wait_recv()

    product = jnp.dot(
        down[...], gathered[...].reshape(N, 256), preferred_element_type=jnp.float32
    )
    deep = product.shape[0] // 4
    product = product[: 2 * deep] + product[2 * deep :]
    real = (product[:deep, :128] - product[deep:, 128:]).astype(jnp.bfloat16)
    imag = (product[:deep, 128:] + product[deep:, :128]).astype(jnp.bfloat16)
    core[:deep, :128] = real
    core[:deep, 128:] = imag
    core[deep:, :128] = -imag
    core[deep:, 128:] = real
    for load in loads[11:]:
        load.wait()
    for copy in copies + shares + hops:
        copy.wait_send()


def probe_kernel(
    beam_y_hbm,
    beam_x_hbm,
    core,
    coefficient,
    spread_y,
    spread_x,
    out,
    beam_y,
    beam_x,
    half,
    field_re,
    field_im,
    beam_sem,
):
    loads = [
        pltpu.make_async_copy(beam_y_hbm, beam_y, beam_sem.at[0]),
        pltpu.make_async_copy(beam_x_hbm, beam_x, beam_sem.at[1]),
    ]
    for load in loads:
        load.start()

    middle = core[...]

    def tilts(step, carry):
        rows = pl.ds(pl.multiple_of(step * 192, 192), 192)
        half[rows, :] = jnp.dot(
            spread_y[rows, :], middle, preferred_element_type=jnp.float32
        ).astype(jnp.bfloat16)
        return carry

    lax.fori_loop(0, KINDS * TILE_Y // 192, tilts, 0)

    for load in loads:
        load.wait()
    group = lax.broadcasted_iota(jnp.int32, (16, 128), 1) // 32
    even = (group & 1) == 0

    def one_beam(beam):
        rows = pl.ds(pl.multiple_of((beam_y[beam] + TILT) * TILE_Y, TILE_Y), TILE_Y)
        value = jnp.dot(
            half[rows, :], spread_x[beam_x[beam] + TILT], preferred_element_type=jnp.float32
        )
        a, b, c, d = (value[16 * i : 16 * i + 16] for i in range(4))
        straight = jnp.where(
            group < 2, jnp.where(group == 0, a, b), jnp.where(group == 2, c, d)
        )
        crossed = jnp.where(
            group < 2, jnp.where(group == 0, b, a), jnp.where(group == 2, d, c)
        )
        crossed = jnp.where(even, pltpu.roll(crossed, 96, 1), pltpu.roll(crossed, 32, 1))
        rows = pl.ds(pl.multiple_of(beam * 16, 16), 16)
        field_re[rows, :] = jnp.where(even, straight, crossed)
        field_im[rows, :] = jnp.where(even, crossed, straight)

    def beams(step, carry):
        for inner in range(8):
            one_beam(step * 8 + inner)
        return carry

    lax.fori_loop(0, 16, beams, 0)

    for piece in range(16):
        rows = pl.ds(piece, 128, stride=16)
        field = jnp.concatenate([field_re[rows, :], field_im[rows, :]], axis=1)
        field = field.astype(jnp.bfloat16)
        product = jnp.dot(coefficient[...], field, preferred_element_type=jnp.float32)
        real = product[:128, :128] - product[128:, 128:]
        imag = product[:128, 128:] + product[128:, :128]
        out[:, 128 * piece : 128 * piece + 128] = real * real + imag * imag


def body(
    atom_y, atom_x, atom_weight, beam_ky, beam_kx, beam_amplitude, crop_offset, probe_y, probe_x
):
    across, down, spread_y, spread_x = (jnp.asarray(v) for v in tables())
    vmem = pl.BlockSpec(memory_space=pltpu.VMEM)
    hbm = pl.BlockSpec(memory_space=pltpu.HBM)
    bf16 = jnp.bfloat16
    stay = functools.partial(pltpu.with_memory_space_constraint, memory_space=pltpu.HBM)
    core, coefficient, spread_y, spread_x = pl.pallas_call(
        potential_kernel,
        name="potential_to_basis",
        out_shape=[
            jax.ShapeDtypeStruct((384, 256), bf16),
            jax.ShapeDtypeStruct((256, 128), bf16),
            jax.ShapeDtypeStruct(spread_y.shape, bf16),
            jax.ShapeDtypeStruct(spread_x.shape, bf16),
        ],
        in_specs=[hbm] * 13,
        out_specs=[vmem] * 4,
        scratch_shapes=[
            pltpu.SMEM((2,), jnp.int32),
            pltpu.VMEM((3, 32, 128), jnp.float32),
            pltpu.VMEM((4, 1, 128), jnp.int32),
            pltpu.VMEM((1, 128), jnp.float32),
            pltpu.VMEM((128 * GROUPS, N), bf16),
            pltpu.VMEM((BAND_ROWS, 128 * GROUPS), bf16),
            pltpu.VMEM((CHUNKS, COLS, 16, SLICE_WIDE), bf16),
            pltpu.VMEM((CHUNKS, COLS, 16, SLICE_WIDE), bf16),
            pltpu.VMEM((CHUNKS, COLS, 16, SLICE_WIDE), bf16),
            pltpu.VMEM((2 * CHUNK_ROWS, N), bf16),
            pltpu.VMEM((N, 512), bf16),
            pltpu.VMEM((768, N), bf16),
            pltpu.VMEM((BAND_ROWS // PIECE, PIECE, 256), bf16),
            pltpu.VMEM((N // PIECE, PIECE, 256), bf16),
            pltpu.SemaphoreType.DMA((13,)),
            pltpu.SemaphoreType.DMA((CHUNKS, COLS)),
            pltpu.SemaphoreType.DMA((CHUNKS, COLS)),
            pltpu.SemaphoreType.DMA((CHUNKS, COLS)),
            pltpu.SemaphoreType.DMA((CHUNKS, COLS)),
            pltpu.SemaphoreType.DMA((BAND_ROWS // PIECE, ROWS)),
            pltpu.SemaphoreType.DMA((BAND_ROWS // PIECE, ROWS)),
        ],
        compiler_params=pltpu.CompilerParams(
            collective_id=0, has_side_effects=True, vmem_limit_bytes=24 * 2**20
        ),
    )(
        stay(crop_offset),
        stay(atom_y.reshape(32, 128)),
        stay(atom_x.reshape(32, 128)),
        stay(atom_weight.reshape(32, 128)),
        stay(beam_ky.reshape(1, 128)),
        stay(beam_kx.reshape(1, 128)),
        stay(beam_amplitude.reshape(1, 128)),
        stay(probe_y.reshape(1, 128)),
        stay(probe_x.reshape(1, 128)),
        stay(across),
        stay(down),
        stay(spread_y),
        stay(spread_x),
    )
    result = pl.pallas_call(
        probe_kernel,
        name="basis_to_probes",
        out_shape=jax.ShapeDtypeStruct((128, 2048), jnp.float32),
        in_specs=[hbm] * 2 + [vmem] * 4,
        out_specs=vmem,
        scratch_shapes=[
            pltpu.SMEM((128,), jnp.int32),
            pltpu.SMEM((128,), jnp.int32),
            pltpu.VMEM((KINDS * TILE_Y, 256), bf16),
            pltpu.VMEM((128 * 16, 128), jnp.float32),
            pltpu.VMEM((128 * 16, 128), jnp.float32),
            pltpu.SemaphoreType.DMA((2,)),
        ],
        compiler_params=pltpu.CompilerParams(vmem_limit_bytes=24 * 2**20),
    )(stay(beam_ky), stay(beam_kx), core, coefficient, spread_y, spread_x)
    return result[None, None]


def solution(mesh):
    return jax.shard_map(
        body,
        mesh=mesh,
        in_specs=(
            P("col"),
            P("col"),
            P("col"),
            P(),
            P(),
            P(),
            P(),
            P("row", "col", None),
            P("row", "col", None),
        ),
        out_specs=P("row", "col", None, None),
        check_vma=False,
    )
```

```python
import functools
import math

import jax
import jax.numpy as jnp
import numpy as np
from jax import lax
from jax.experimental import pallas as pl
from jax.experimental.pallas import tpu as pltpu
from jax.sharding import PartitionSpec as P

N = 1024
WIN = 512
ROWS = 8
COLS = 16
TILT = 16
KINDS = 2 * TILT + 1
TILE_Y = WIN // ROWS
TILE_X = WIN // COLS
BAND_ROWS = N // ROWS
GROUPS = 7
CHUNKS = 2
UNROLL = 64
CHUNK_ROWS = BAND_ROWS // CHUNKS
SLICE_HIGH = CHUNK_ROWS // 16
SLICE_WIDE = N * SLICE_HIGH // COLS
LEAD = TILE_X * (COLS - 1)
MESH = pl.DeviceIdType.MESH


EDGE = np.concatenate([np.arange(N // 2 - TILT, N // 2), np.arange(-N // 2, -N // 2 + TILT)])
EDGES = (EDGE[EDGE % 2 != 0], EDGE[EDGE % 2 == 0])


def turn(number, modulus):
    return np.exp(2j * np.pi * np.mod(number, modulus) / modulus)


def fresnel():
    freq = np.arange(-N // 2, N // 2)
    half = np.arange(2 * N)
    return (turn(np.outer(half, freq), 2 * N) * turn(-freq * freq, 4 * N)[None, :]).sum(1) / N


def basis(length):
    table = fresnel()
    place = np.arange(N)
    shift = np.arange(length + TILT)
    rows = []
    for odd in (0, 1):
        apart = 2 * (shift[:, None] - TILT // 2 - place[None, :]) + odd
        edge = EDGES[odd]
        rows.append(table[np.mod(apart, 2 * N)])
        rows.append(turn(-edge * edge, 4 * N)[:, None] * turn(-np.outer(edge, place), N) / N)
    return np.concatenate(rows)


def synthesis(length):
    count = length + TILT
    pixel = np.arange(length)
    out = np.zeros((KINDS, length, count + TILT), complex)
    for kind in range(KINDS):
        tilt = kind - TILT
        odd = tilt % 2
        phase = turn(tilt * pixel, N)
        out[kind, pixel, pixel - (tilt + odd) // 2 + TILT // 2] = phase
        moved = EDGES[odd] + tilt
        flips = (moved < -N // 2) | (moved >= N // 2)
        wrapped = -2 * turn((2 * pixel[:, None] - tilt) * EDGES[odd][None, :], 2 * N)
        out[kind, :, count:] = phase[:, None] * np.where(flips[None, :], wrapped, 0)
    return out


def two_parts(value, axis):
    high = value.astype(jnp.bfloat16).astype(np.float64)
    return np.concatenate([high, value - high], axis)


@functools.lru_cache(None)
def tables():
    across = basis(TILE_X).T
    across = two_parts(np.concatenate([across.real, across.imag], 1), 1)
    across = np.concatenate([across[N - LEAD :], across], 0)
    down = basis(TILE_Y)
    down = two_parts(np.concatenate([down.real, down.imag], 0), 0)
    down = down.reshape(-1, ROWS, 2, TILE_Y).transpose(2, 0, 1, 3)
    down = down.reshape(2, down.shape[1], ROWS * TILE_Y)
    spread_y = synthesis(TILE_Y)
    order = (4 * np.arange(TILE_Y // 4)[None, :] + np.arange(4)[:, None]).reshape(-1)
    spread_y = np.concatenate([spread_y[0::2], spread_y[1::2]])[:, order]
    spread_y = np.concatenate([spread_y.real, spread_y.imag], 2).reshape(KINDS * TILE_Y, -1)
    spread_x = synthesis(TILE_X).transpose(0, 2, 1)
    top = np.concatenate([spread_x.real, spread_x.imag], 2)
    bottom = np.concatenate([-spread_x.imag, spread_x.real], 2)
    spread_x = np.concatenate([top, bottom], 1)
    spread_x = np.concatenate([spread_x, spread_x], 2)
    return tuple(
        value.astype(jnp.bfloat16) for value in (across, down, spread_y, spread_x)
    )


@functools.lru_cache(None)
def wave_fit():
    grid = np.cos(np.pi * (np.arange(4000) + 0.5) / 4000) * np.pi
    square = grid * grid
    powers = (square / np.pi**2)[:, None] ** np.arange(8)[None, :]
    even = np.linalg.lstsq(powers, np.cos(grid), rcond=None)[0] / np.pi ** (2 * np.arange(8))
    odd = np.linalg.lstsq(powers, np.sin(grid) / grid, rcond=None)[0] / np.pi ** (2 * np.arange(8))
    return [float(v) for v in even], [float(v) for v in odd]


def cos_sin_reduced(angle):
    even, odd = wave_fit()
    square = angle * angle
    cosine = jnp.full_like(angle, even[-1])
    sine = jnp.full_like(angle, odd[-1])
    for e, o in zip(even[-2::-1], odd[-2::-1]):
        cosine = cosine * square + e
        sine = sine * square + o
    return cosine, sine * angle


TURN_A = 6.28125
TURN_B = 0.0019350051879882812
TURN_C = 2.0 * math.pi - TURN_A - TURN_B


def cos_sin(angle):
    whole = jnp.floor(angle * (0.5 / math.pi) + 0.5)
    return cos_sin_reduced(((angle - whole * TURN_A) - whole * TURN_B) - whole * TURN_C)


def slice_place(block):
    high, side = block % SLICE_HIGH, block // SLICE_HIGH
    return (
        slice(16 * high, 16 * high + 16),
        slice(SLICE_WIDE * side, SLICE_WIDE * side + SLICE_WIDE),
    )


def potential_kernel(
    crop_hbm,
    atom_y_hbm,
    atom_x_hbm,
    atom_weight_hbm,
    tilt_y_hbm,
    tilt_x_hbm,
    amplitude_hbm,
    probe_y_hbm,
    probe_x_hbm,
    across_hbm,
    down_hbm,
    spread_y_hbm,
    spread_x_hbm,
    core,
    coefficient,
    spread_y,
    spread_x,
    crop,
    atoms,
    beams,
    amplitude,
    prof_x,
    prof_y,
    part,
    landed,
    whole,
    wave,
    across,
    down,
    moved,
    gathered,
    table_sem,
    part_send,
    part_recv,
    whole_send,
    whole_recv,
    moved_send,
    moved_recv,
):
    row = lax.axis_index("row")
    col = lax.axis_index("col")
    start = pl.multiple_of(LEAD - TILE_X * col, TILE_X)
    loads = [
        pltpu.make_async_copy(source, target, table_sem.at[place])
        for place, (source, target) in enumerate(
            (
                (crop_hbm, crop),
                (atom_y_hbm, atoms.at[0]),
                (atom_x_hbm, atoms.at[1]),
                (atom_weight_hbm, atoms.at[2]),
                (tilt_y_hbm, beams.at[0]),
                (tilt_x_hbm, beams.at[1]),
                (probe_y_hbm, beams.at[2]),
                (probe_x_hbm, beams.at[3]),
                (amplitude_hbm, amplitude),
                (across_hbm.at[pl.ds(start, N)], across),
                (down_hbm, down),
                (spread_y_hbm, spread_y),
                (spread_x_hbm, spread_x),
            )
        )
    ]
    for load in loads[:4]:
        load.start()
    barrier = pltpu.get_barrier_semaphore()
    for step in range(1, COLS):
        peer = lax.rem(col + step, COLS)
        pl.semaphore_signal(barrier, inc=1, device_id={"col": peer}, device_id_type=MESH)
    for step in range(1, ROWS):
        peer = lax.rem(row + step, ROWS)
        pl.semaphore_signal(barrier, inc=1, device_id={"row": peer}, device_id_type=MESH)
    for load in loads[4:9]:
        load.start()
    for load in loads[:4]:
        load.wait()

    crop_y = crop[0]
    crop_x = crop[1]
    first_y = (BAND_ROWS * row + crop_y) & (N - 1)
    first_group = ((first_y + (N - 21)) & (N - 1)) // 32
    at_y = ((lax.broadcasted_iota(jnp.int32, (BAND_ROWS, 128), 0) + first_y) & (N - 1)).astype(
        jnp.float32
    )
    lane = lax.broadcasted_iota(jnp.int32, (128, N), 1)
    at_x = ((lane + crop_x) & (N - 1)).astype(jnp.float32)
    for group in range(GROUPS):
        index = (first_group + group) & 31
        here_y = atoms[0, pl.ds(index, 1), :]
        here_x = atoms[1, pl.ds(index, 1), :]
        here_w = atoms[2, pl.ds(index, 1), :]
        apart = (at_y - here_y) * 0.5
        value = jnp.exp(-(apart * apart)) * here_w
        prof_y[:, 128 * group : 128 * group + 128] = value.astype(jnp.bfloat16)
        column = jnp.transpose(jnp.broadcast_to(here_x, (128, 128)))
        column = jnp.concatenate([column] * (N // 128), axis=1)
        apart = (at_x - column) * 0.5
        prof_x[128 * group : 128 * group + 128, :] = jnp.exp(-(apart * apart)).astype(jnp.bfloat16)
    partial = jnp.dot(prof_y[...], prof_x[...], preferred_element_type=jnp.float32)
    for chunk in range(CHUNKS):
        rows = partial[CHUNK_ROWS * chunk : CHUNK_ROWS * chunk + CHUNK_ROWS].astype(jnp.bfloat16)
        for block in range(COLS):
            part[chunk, block] = rows[slice_place(block)]
    pl.semaphore_wait(barrier, COLS - 1 + ROWS - 1)

    copies = []
    for chunk in range(CHUNKS):
        for step in range(1, COLS):
            peer = lax.rem(col + step, COLS)
            copy = pltpu.make_async_remote_copy(
                src_ref=part.at[chunk, peer],
                dst_ref=landed.at[chunk, step],
                send_sem=part_send.at[chunk, step],
                recv_sem=part_recv.at[chunk, step],
                device_id={"col": peer},
                device_id_type=MESH,
            )
            copy.start()
            copies.append(copy)

    for load in loads[9:]:
        load.start()

    for load in loads[4:9]:
        load.wait()
    ky = beams[0]
    kx = beams[1]
    at_y = jnp.transpose(jnp.broadcast_to(beams[2], (128, 128))) - TILE_Y * row
    at_x = jnp.transpose(jnp.broadcast_to(beams[3], (128, 128))) - TILE_X * col
    number = (4 * (ky * at_y + kx * at_x) + ky * ky + kx * kx) & (4 * N - 1)
    number = jnp.where(number >= 2 * N, number - 4 * N, number)
    real, imag = cos_sin_reduced(number.astype(jnp.float32) * (-2.0 * math.pi / (4 * N)))
    weight = amplitude[...] * (1.0 / math.sqrt(128.0))
    coefficient[:128] = (real * weight).astype(jnp.bfloat16)
    coefficient[128:] = (imag * weight).astype(jnp.bfloat16)

    shares = []
    for chunk in range(CHUNKS):
        total = part[chunk, col].astype(jnp.float32)
        for step in range(1, COLS):
            copies[(COLS - 1) * chunk + step - 1].wait_recv()
            total = total + landed[chunk, step].astype(jnp.float32)
        whole[chunk, col] = (total - 1.0).astype(jnp.bfloat16)
        for step in range(1, COLS):
            peer = lax.rem(col + step, COLS)
            share = pltpu.make_async_remote_copy(
                src_ref=whole.at[chunk, col],
                dst_ref=whole.at[chunk, col],
                send_sem=whole_send.at[chunk, step],
                recv_sem=whole_recv.at[chunk, step],
                device_id={"col": peer},
                device_id_type=MESH,
            )
            share.start()
            shares.append(share)

    loads[9].wait()
    hops = []
    for chunk in range(CHUNKS):
        for share in shares[(COLS - 1) * chunk : (COLS - 1) * (chunk + 1)]:
            share.wait_recv()
        for block in range(COLS):
            rows, columns = slice_place(block)
            real, imag = cos_sin(whole[chunk, block].astype(jnp.float32) + 1.0)
            wave[rows, columns] = real.astype(jnp.bfloat16)
            wave[slice(CHUNK_ROWS + rows.start, CHUNK_ROWS + rows.stop), columns] = imag.astype(
                jnp.bfloat16
            )
        product = jnp.dot(wave[...], across[...], preferred_element_type=jnp.float32)
        product = product[:, :256] + product[:, 256:]
        real = product[:CHUNK_ROWS, :128] - product[CHUNK_ROWS:, 128:]
        imag = product[:CHUNK_ROWS, 128:] + product[CHUNK_ROWS:, :128]
        both = jnp.concatenate([real, imag], axis=1).astype(jnp.bfloat16)
        moved[chunk] = both
        for step in range(1, ROWS):
            peer = lax.rem(row + step, ROWS)
            hop = pltpu.make_async_remote_copy(
                src_ref=moved.at[chunk],
                dst_ref=gathered.at[chunk, ((2 * row + chunk - peer + 16) & 15) // 2],
                send_sem=moved_send.at[chunk, step],
                recv_sem=moved_recv.at[chunk, step],
                device_id={"row": peer},
                device_id_type=MESH,
            )
            hop.start()
            hops.append(hop)
        gathered[chunk, ((row + chunk) & 15) // 2] = both

    loads[10].wait()
    product = None
    for chunk in range(CHUNKS):
        for hop in hops[(ROWS - 1) * chunk : (ROWS - 1) * (chunk + 1)]:
            hop.wait_recv()
        term = jnp.dot(
            down[(row + chunk) & 1],
            gathered[chunk].reshape(ROWS * TILE_Y, 256),
            preferred_element_type=jnp.float32,
        )
        product = term if product is None else product + term
    deep = product.shape[0] // 4
    product = product[: 2 * deep] + product[2 * deep :]
    real = product[:deep, :128] - product[deep:, 128:]
    imag = product[:deep, 128:] + product[deep:, :128]
    lower = lax.broadcasted_iota(jnp.int32, (deep, 128), 1) < 64
    real_turned = pltpu.roll(real, 64, 1)
    imag_turned = pltpu.roll(imag, 64, 1)
    rows = deep // 2
    for side, (first, second) in enumerate(
        (
            (jnp.where(lower, real, imag_turned), jnp.where(lower, -imag, real_turned)),
            (jnp.where(lower, real_turned, imag), jnp.where(lower, -imag_turned, real)),
        )
    ):
        for odd in (0, 1):
            mine = slice(rows * odd, rows * odd + rows)
            lanes = slice(128 * side, 128 * side + 128)
            core[odd, :rows, lanes] = first[mine].astype(jnp.bfloat16)
            core[odd, rows:, lanes] = second[mine].astype(jnp.bfloat16)
    for load in loads[11:]:
        load.wait()
    for copy in copies + shares + hops:
        copy.wait_send()


def probe_kernel(
    beam_y_hbm,
    beam_x_hbm,
    core,
    coefficient,
    spread_y,
    spread_x,
    out,
    beam_y,
    beam_x,
    half,
    field_re,
    field_im,
    result,
    beam_sem,
):
    loads = [
        pltpu.make_async_copy(beam_y_hbm, beam_y, beam_sem.at[0]),
        pltpu.make_async_copy(beam_x_hbm, beam_x, beam_sem.at[1]),
    ]
    for load in loads:
        load.start()

    middle = (KINDS // 2 + 1) * TILE_Y
    for odd, rows in enumerate((slice(0, middle), slice(middle, KINDS * TILE_Y))):
        value = jnp.dot(spread_y[rows], core[odd], preferred_element_type=jnp.float32)
        value = value.astype(jnp.bfloat16)
        half[0, rows] = value[:, :128]
        half[1, rows] = value[:, 128:]

    for load in loads:
        load.wait()
    group = lax.broadcasted_iota(jnp.int32, (16, 128), 1) // 32
    even = (group & 1) == 0

    def one_beam(beam):
        tilt = beam_y[beam]
        other = beam_x[beam]
        kind = (tilt & 1) * (KINDS // 2 + 1) + (tilt + TILT) // 2
        rows = pl.ds(pl.multiple_of(kind * TILE_Y, TILE_Y), TILE_Y)
        value = jnp.dot(
            half[other & 1, rows, :], spread_x[other + TILT], preferred_element_type=jnp.float32
        )
        a, b, c, d = (value[16 * i : 16 * i + 16] for i in range(4))
        straight = jnp.where(
            group < 2, jnp.where(group == 0, a, b), jnp.where(group == 2, c, d)
        )
        crossed = jnp.where(
            group < 2, jnp.where(group == 0, b, a), jnp.where(group == 2, d, c)
        )
        crossed = jnp.where(even, pltpu.roll(crossed, 96, 1), pltpu.roll(crossed, 32, 1))
        rows = pl.ds(pl.multiple_of(beam * 16, 16), 16)
        field_re[rows, :] = jnp.where(even, straight, crossed)
        field_im[rows, :] = jnp.where(even, crossed, straight)

    def beams(step, carry):
        for inner in range(UNROLL):
            one_beam(step * UNROLL + inner)
        return carry

    lax.fori_loop(0, 128 // UNROLL, beams, 0)
    stores = []
    for piece in range(16):
        rows = pl.ds(piece, 128, stride=16)
        field = jnp.concatenate([field_re[rows, :], field_im[rows, :]], axis=1)
        field = field.astype(jnp.bfloat16)
        product = jnp.dot(coefficient[...], field, preferred_element_type=jnp.float32)
        real = product[:128, :128] - product[128:, 128:]
        imag = product[:128, 128:] + product[128:, :128]
        result[:, 128 * piece : 128 * piece + 128] = real * real + imag * imag
        if piece % 4 == 3:
            lanes = pl.ds(128 * (piece - 3), 512)
            store = pltpu.make_async_copy(
                result.at[:, lanes], out.at[:, lanes], beam_sem.at[2 + piece // 4]
            )
            store.start()
            stores.append(store)
    for store in stores:
        store.wait()


def body(
    atom_y, atom_x, atom_weight, beam_ky, beam_kx, beam_amplitude, crop_offset, probe_y, probe_x
):
    across, down, spread_y, spread_x = (jnp.asarray(v) for v in tables())
    vmem = pl.BlockSpec(memory_space=pltpu.VMEM)
    hbm = pl.BlockSpec(memory_space=pltpu.HBM)
    bf16 = jnp.bfloat16
    stay = functools.partial(pltpu.with_memory_space_constraint, memory_space=pltpu.HBM)
    core, coefficient, spread_y, spread_x = pl.pallas_call(
        potential_kernel,
        name="potential_to_basis",
        out_shape=[
            jax.ShapeDtypeStruct((2, 192, 256), bf16),
            jax.ShapeDtypeStruct((256, 128), bf16),
            jax.ShapeDtypeStruct(spread_y.shape, bf16),
            jax.ShapeDtypeStruct(spread_x.shape, bf16),
        ],
        in_specs=[hbm] * 13,
        out_specs=[vmem] * 4,
        scratch_shapes=[
            pltpu.SMEM((2,), jnp.int32),
            pltpu.VMEM((3, 32, 128), jnp.float32),
            pltpu.VMEM((4, 1, 128), jnp.int32),
            pltpu.VMEM((1, 128), jnp.float32),
            pltpu.VMEM((128 * GROUPS, N), bf16),
            pltpu.VMEM((BAND_ROWS, 128 * GROUPS), bf16),
            pltpu.VMEM((CHUNKS, COLS, 16, SLICE_WIDE), bf16),
            pltpu.VMEM((CHUNKS, COLS, 16, SLICE_WIDE), bf16),
            pltpu.VMEM((CHUNKS, COLS, 16, SLICE_WIDE), bf16),
            pltpu.VMEM((2 * CHUNK_ROWS, N), bf16),
            pltpu.VMEM((N, 512), bf16),
            pltpu.VMEM((2, 768, ROWS * TILE_Y), bf16),
            pltpu.VMEM((CHUNKS, CHUNK_ROWS, 256), bf16),
            pltpu.VMEM((CHUNKS, ROWS, CHUNK_ROWS, 256), bf16),
            pltpu.SemaphoreType.DMA((13,)),
            pltpu.SemaphoreType.DMA((CHUNKS, COLS)),
            pltpu.SemaphoreType.DMA((CHUNKS, COLS)),
            pltpu.SemaphoreType.DMA((CHUNKS, COLS)),
            pltpu.SemaphoreType.DMA((CHUNKS, COLS)),
            pltpu.SemaphoreType.DMA((CHUNKS, ROWS)),
            pltpu.SemaphoreType.DMA((CHUNKS, ROWS)),
        ],
        compiler_params=pltpu.CompilerParams(
            collective_id=0, has_side_effects=True, vmem_limit_bytes=24 * 2**20
        ),
    )(
        stay(crop_offset),
        stay(atom_y.reshape(32, 128)),
        stay(atom_x.reshape(32, 128)),
        stay(atom_weight.reshape(32, 128)),
        stay(beam_ky.reshape(1, 128)),
        stay(beam_kx.reshape(1, 128)),
        stay(beam_amplitude.reshape(1, 128)),
        stay(probe_y.reshape(1, 128)),
        stay(probe_x.reshape(1, 128)),
        stay(across),
        stay(down),
        stay(spread_y),
        stay(spread_x),
    )
    result = pl.pallas_call(
        probe_kernel,
        name="basis_to_probes",
        out_shape=jax.ShapeDtypeStruct((128, 2048), jnp.float32),
        in_specs=[hbm] * 2 + [vmem] * 4,
        out_specs=hbm,
        scratch_shapes=[
            pltpu.SMEM((128,), jnp.int32),
            pltpu.SMEM((128,), jnp.int32),
            pltpu.VMEM((2, KINDS * TILE_Y, 128), bf16),
            pltpu.VMEM((128 * 16, 128), jnp.float32),
            pltpu.VMEM((128 * 16, 128), jnp.float32),
            pltpu.VMEM((128, 2048), jnp.float32),
            pltpu.SemaphoreType.DMA((6,)),
        ],
        compiler_params=pltpu.CompilerParams(vmem_limit_bytes=24 * 2**20),
    )(stay(beam_ky), stay(beam_kx), core, coefficient, spread_y, spread_x)
    return result[None, None]


def solution(mesh):
    return jax.shard_map(
        body,
        mesh=mesh,
        in_specs=(
            P("col"),
            P("col"),
            P("col"),
            P(),
            P(),
            P(),
            P(),
            P("row", "col", None),
            P("row", "col", None),
        ),
        out_specs=P("row", "col", None, None),
        check_vma=False,
    )
```

```python
import functools
import math

import jax
import jax.numpy as jnp
import numpy as np
from jax import lax
from jax.experimental import pallas as pl
from jax.experimental.pallas import tpu as pltpu
from jax.sharding import PartitionSpec as P

N = 1024
WIN = 512
ROWS = 8
COLS = 16
TILT = 16
KINDS = 2 * TILT + 1
TILE_Y = WIN // ROWS
TILE_X = WIN // COLS
BAND_ROWS = N // ROWS
GROUPS = 7
CHUNKS = 2
UNROLL = 128
CHUNK_ROWS = BAND_ROWS // CHUNKS
SLICE_HIGH = CHUNK_ROWS // 16
SLICE_WIDE = N * SLICE_HIGH // COLS
LEAD = TILE_X * (COLS - 1)
MESH = pl.DeviceIdType.MESH


EDGE = np.concatenate([np.arange(N // 2 - TILT, N // 2), np.arange(-N // 2, -N // 2 + TILT)])
EDGES = (EDGE[EDGE % 2 != 0], EDGE[EDGE % 2 == 0])


def turn(number, modulus):
    return np.exp(2j * np.pi * np.mod(number, modulus) / modulus)


def fresnel():
    freq = np.arange(-N // 2, N // 2)
    half = np.arange(2 * N)
    return (turn(np.outer(half, freq), 2 * N) * turn(-freq * freq, 4 * N)[None, :]).sum(1) / N


def basis(length):
    table = fresnel()
    place = np.arange(N)
    shift = np.arange(length + TILT)
    rows = []
    for odd in (0, 1):
        apart = 2 * (shift[:, None] - TILT // 2 - place[None, :]) + odd
        edge = EDGES[odd]
        rows.append(table[np.mod(apart, 2 * N)])
        rows.append(turn(-edge * edge, 4 * N)[:, None] * turn(-np.outer(edge, place), N) / N)
    return np.concatenate(rows)


def synthesis(length):
    count = length + TILT
    pixel = np.arange(length)
    out = np.zeros((KINDS, length, count + TILT), complex)
    for kind in range(KINDS):
        tilt = kind - TILT
        odd = tilt % 2
        phase = turn(tilt * pixel, N)
        out[kind, pixel, pixel - (tilt + odd) // 2 + TILT // 2] = phase
        moved = EDGES[odd] + tilt
        flips = (moved < -N // 2) | (moved >= N // 2)
        wrapped = -2 * turn((2 * pixel[:, None] - tilt) * EDGES[odd][None, :], 2 * N)
        out[kind, :, count:] = phase[:, None] * np.where(flips[None, :], wrapped, 0)
    return out


def two_parts(value, axis):
    high = value.astype(jnp.bfloat16).astype(np.float64)
    return np.concatenate([high, value - high], axis)


@functools.lru_cache(None)
def tables():
    across = basis(TILE_X).T
    across = two_parts(np.concatenate([across.real, across.imag], 1), 1)
    across = np.concatenate([across[N - LEAD :], across], 0)
    down = basis(TILE_Y)
    down = two_parts(np.concatenate([down.real, down.imag], 0), 0)
    down = down.reshape(-1, ROWS, 2, TILE_Y).transpose(2, 0, 1, 3)
    down = down.reshape(2, down.shape[1], ROWS * TILE_Y)
    spread_y = synthesis(TILE_Y)
    order = (4 * np.arange(TILE_Y // 4)[None, :] + np.arange(4)[:, None]).reshape(-1)
    spread_y = np.concatenate([spread_y[0::2], spread_y[1::2]])[:, order]
    spread_y = np.concatenate([spread_y.real, spread_y.imag], 2).reshape(KINDS * TILE_Y, -1)
    spread_x = synthesis(TILE_X).transpose(0, 2, 1)
    top = np.concatenate([spread_x.real, spread_x.imag], 2)
    bottom = np.concatenate([-spread_x.imag, spread_x.real], 2)
    spread_x = np.concatenate([top, bottom], 1)
    spread_x = np.concatenate([spread_x, spread_x], 2)
    return tuple(
        value.astype(jnp.bfloat16) for value in (across, down, spread_y, spread_x)
    )


@functools.lru_cache(None)
def wave_fit():
    grid = np.cos(np.pi * (np.arange(4000) + 0.5) / 4000) * np.pi
    square = grid * grid
    powers = (square / np.pi**2)[:, None] ** np.arange(8)[None, :]
    even = np.linalg.lstsq(powers, np.cos(grid), rcond=None)[0] / np.pi ** (2 * np.arange(8))
    odd = np.linalg.lstsq(powers, np.sin(grid) / grid, rcond=None)[0] / np.pi ** (2 * np.arange(8))
    return [float(v) for v in even], [float(v) for v in odd]


def cos_sin_reduced(angle):
    even, odd = wave_fit()
    square = angle * angle
    cosine = jnp.full_like(angle, even[-1])
    sine = jnp.full_like(angle, odd[-1])
    for e, o in zip(even[-2::-1], odd[-2::-1]):
        cosine = cosine * square + e
        sine = sine * square + o
    return cosine, sine * angle


TURN_A = 6.28125
TURN_B = 0.0019350051879882812
TURN_C = 2.0 * math.pi - TURN_A - TURN_B


def cos_sin(angle):
    whole = jnp.floor(angle * (0.5 / math.pi) + 0.5)
    return cos_sin_reduced(((angle - whole * TURN_A) - whole * TURN_B) - whole * TURN_C)


def slice_place(block):
    high, side = block % SLICE_HIGH, block // SLICE_HIGH
    return (
        slice(16 * high, 16 * high + 16),
        slice(SLICE_WIDE * side, SLICE_WIDE * side + SLICE_WIDE),
    )


def potential_kernel(
    crop_hbm,
    atom_y_hbm,
    atom_x_hbm,
    atom_weight_hbm,
    tilt_y_hbm,
    tilt_x_hbm,
    amplitude_hbm,
    probe_y_hbm,
    probe_x_hbm,
    across_hbm,
    down_hbm,
    spread_y_hbm,
    spread_x_hbm,
    core,
    coefficient,
    spread_y,
    spread_x,
    beams,
    crop,
    atoms,
    amplitude,
    prof_x,
    prof_y,
    part,
    landed,
    whole,
    wave,
    across,
    down,
    moved,
    gathered,
    table_sem,
    part_send,
    part_recv,
    whole_send,
    whole_recv,
    moved_send,
    moved_recv,
):
    row = lax.axis_index("row")
    col = lax.axis_index("col")
    start = pl.multiple_of(LEAD - TILE_X * col, TILE_X)
    loads = [
        pltpu.make_async_copy(source, target, table_sem.at[place])
        for place, (source, target) in enumerate(
            (
                (crop_hbm, crop),
                (atom_y_hbm, atoms.at[0]),
                (atom_x_hbm, atoms.at[1]),
                (atom_weight_hbm, atoms.at[2]),
                (tilt_y_hbm, beams.at[0]),
                (tilt_x_hbm, beams.at[1]),
                (probe_y_hbm, beams.at[2]),
                (probe_x_hbm, beams.at[3]),
                (amplitude_hbm, amplitude),
                (across_hbm.at[pl.ds(start, N)], across),
                (down_hbm, down),
                (spread_y_hbm, spread_y),
                (spread_x_hbm, spread_x),
            )
        )
    ]
    for load in loads[:4]:
        load.start()
    barrier = pltpu.get_barrier_semaphore()
    for step in range(1, COLS):
        peer = lax.rem(col + step, COLS)
        pl.semaphore_signal(barrier, inc=1, device_id={"col": peer}, device_id_type=MESH)
    for step in range(1, ROWS):
        peer = lax.rem(row + step, ROWS)
        pl.semaphore_signal(barrier, inc=1, device_id={"row": peer}, device_id_type=MESH)
    for load in loads[4:9]:
        load.start()
    for load in loads[:4]:
        load.wait()

    crop_y = crop[0]
    crop_x = crop[1]
    first_y = (BAND_ROWS * row + crop_y) & (N - 1)
    first_group = ((first_y + (N - 21)) & (N - 1)) // 32
    at_y = ((lax.broadcasted_iota(jnp.int32, (BAND_ROWS, 128), 0) + first_y) & (N - 1)).astype(
        jnp.float32
    )
    lane = lax.broadcasted_iota(jnp.int32, (128, N), 1)
    at_x = ((lane + crop_x) & (N - 1)).astype(jnp.float32)
    for group in range(GROUPS):
        index = (first_group + group) & 31
        here_y = atoms[0, pl.ds(index, 1), :]
        here_x = atoms[1, pl.ds(index, 1), :]
        here_w = atoms[2, pl.ds(index, 1), :]
        apart = (at_y - here_y) * 0.5
        value = jnp.exp(-(apart * apart)) * here_w
        prof_y[:, 128 * group : 128 * group + 128] = value.astype(jnp.bfloat16)
        column = jnp.transpose(jnp.broadcast_to(here_x, (128, 128)))
        column = jnp.concatenate([column] * (N // 128), axis=1)
        apart = (at_x - column) * 0.5
        prof_x[128 * group : 128 * group + 128, :] = jnp.exp(-(apart * apart)).astype(jnp.bfloat16)
    partial = jnp.dot(prof_y[...], prof_x[...], preferred_element_type=jnp.float32)
    for chunk in range(CHUNKS):
        rows = partial[CHUNK_ROWS * chunk : CHUNK_ROWS * chunk + CHUNK_ROWS].astype(jnp.bfloat16)
        for block in range(COLS):
            part[chunk, block] = rows[slice_place(block)]
    pl.semaphore_wait(barrier, COLS - 1 + ROWS - 1)

    copies = []
    for chunk in range(CHUNKS):
        for step in range(1, COLS):
            peer = lax.rem(col + step, COLS)
            copy = pltpu.make_async_remote_copy(
                src_ref=part.at[chunk, peer],
                dst_ref=landed.at[chunk, step],
                send_sem=part_send.at[chunk, step],
                recv_sem=part_recv.at[chunk, step],
                device_id={"col": peer},
                device_id_type=MESH,
            )
            copy.start()
            copies.append(copy)

    for load in loads[9:]:
        load.start()

    for load in loads[4:9]:
        load.wait()
    ky = beams[0]
    kx = beams[1]
    at_y = jnp.transpose(jnp.broadcast_to(beams[2], (128, 128))) - TILE_Y * row
    at_x = jnp.transpose(jnp.broadcast_to(beams[3], (128, 128))) - TILE_X * col
    number = (4 * (ky * at_y + kx * at_x) + ky * ky + kx * kx) & (4 * N - 1)
    number = jnp.where(number >= 2 * N, number - 4 * N, number)
    real, imag = cos_sin_reduced(number.astype(jnp.float32) * (-2.0 * math.pi / (4 * N)))
    weight = amplitude[...] * (1.0 / math.sqrt(128.0))
    coefficient[:128] = (real * weight).astype(jnp.bfloat16)
    coefficient[128:] = (imag * weight).astype(jnp.bfloat16)

    shares = []
    for chunk in range(CHUNKS):
        total = part[chunk, col].astype(jnp.float32)
        for step in range(1, COLS):
            copies[(COLS - 1) * chunk + step - 1].wait_recv()
            total = total + landed[chunk, step].astype(jnp.float32)
        whole[chunk, col] = (total - 1.0).astype(jnp.bfloat16)
        for step in range(1, COLS):
            peer = lax.rem(col + step, COLS)
            share = pltpu.make_async_remote_copy(
                src_ref=whole.at[chunk, col],
                dst_ref=whole.at[chunk, col],
                send_sem=whole_send.at[chunk, step],
                recv_sem=whole_recv.at[chunk, step],
                device_id={"col": peer},
                device_id_type=MESH,
            )
            share.start()
            shares.append(share)

    loads[9].wait()
    hops = []
    for chunk in range(CHUNKS):
        for share in shares[(COLS - 1) * chunk : (COLS - 1) * (chunk + 1)]:
            share.wait_recv()
        for block in range(COLS):
            rows, columns = slice_place(block)
            real, imag = cos_sin(whole[chunk, block].astype(jnp.float32) + 1.0)
            wave[rows, columns] = real.astype(jnp.bfloat16)
            wave[slice(CHUNK_ROWS + rows.start, CHUNK_ROWS + rows.stop), columns] = imag.astype(
                jnp.bfloat16
            )
        product = jnp.dot(wave[...], across[...], preferred_element_type=jnp.float32)
        product = product[:, :256] + product[:, 256:]
        real = product[:CHUNK_ROWS, :128] - product[CHUNK_ROWS:, 128:]
        imag = product[:CHUNK_ROWS, 128:] + product[CHUNK_ROWS:, :128]
        both = jnp.concatenate([real, imag], axis=1).astype(jnp.bfloat16)
        moved[chunk] = both
        for step in range(1, ROWS):
            peer = lax.rem(row + step, ROWS)
            hop = pltpu.make_async_remote_copy(
                src_ref=moved.at[chunk],
                dst_ref=gathered.at[chunk, ((2 * row + chunk - peer + 16) & 15) // 2],
                send_sem=moved_send.at[chunk, step],
                recv_sem=moved_recv.at[chunk, step],
                device_id={"row": peer},
                device_id_type=MESH,
            )
            hop.start()
            hops.append(hop)
        gathered[chunk, ((row + chunk) & 15) // 2] = both

    loads[10].wait()
    product = None
    for chunk in range(CHUNKS):
        for hop in hops[(ROWS - 1) * chunk : (ROWS - 1) * (chunk + 1)]:
            hop.wait_recv()
        term = jnp.dot(
            down[(row + chunk) & 1],
            gathered[chunk].reshape(ROWS * TILE_Y, 256),
            preferred_element_type=jnp.float32,
        )
        product = term if product is None else product + term
    deep = product.shape[0] // 4
    product = product[: 2 * deep] + product[2 * deep :]
    real = product[:deep, :128] - product[deep:, 128:]
    imag = product[:deep, 128:] + product[deep:, :128]
    lower = lax.broadcasted_iota(jnp.int32, (deep, 128), 1) < 64
    real_turned = pltpu.roll(real, 64, 1)
    imag_turned = pltpu.roll(imag, 64, 1)
    rows = deep // 2
    for side, (first, second) in enumerate(
        (
            (jnp.where(lower, real, imag_turned), jnp.where(lower, -imag, real_turned)),
            (jnp.where(lower, real_turned, imag), jnp.where(lower, -imag_turned, real)),
        )
    ):
        for odd in (0, 1):
            mine = slice(rows * odd, rows * odd + rows)
            lanes = slice(128 * side, 128 * side + 128)
            core[odd, :rows, lanes] = first[mine].astype(jnp.bfloat16)
            core[odd, rows:, lanes] = second[mine].astype(jnp.bfloat16)
    for load in loads[11:]:
        load.wait()
    for copy in copies + shares + hops:
        copy.wait_send()


def probe_kernel(
    beams,
    core,
    coefficient,
    spread_y,
    spread_x,
    out,
    tilts,
    half,
    field_re,
    field_im,
    result,
    beam_sem,
):
    load = pltpu.make_async_copy(beams.at[pl.ds(0, 2)], tilts, beam_sem.at[0])
    load.start()

    middle = (KINDS // 2 + 1) * TILE_Y
    for odd, rows in enumerate((slice(0, middle), slice(middle, KINDS * TILE_Y))):
        value = jnp.dot(spread_y[rows], core[odd], preferred_element_type=jnp.float32)
        value = value.astype(jnp.bfloat16)
        half[0, rows] = value[:, :128]
        half[1, rows] = value[:, 128:]

    load.wait()
    group = lax.broadcasted_iota(jnp.int32, (16, 128), 1) // 32
    even = (group & 1) == 0

    def one_beam(beam):
        tilt = tilts[0, 0, beam]
        other = tilts[1, 0, beam]
        kind = (tilt & 1) * (KINDS // 2 + 1) + (tilt + TILT) // 2
        rows = pl.ds(pl.multiple_of(kind * TILE_Y, TILE_Y), TILE_Y)
        value = jnp.dot(
            half[other & 1, rows, :], spread_x[other + TILT], preferred_element_type=jnp.float32
        )
        a, b, c, d = (value[16 * i : 16 * i + 16] for i in range(4))
        straight = jnp.where(
            group < 2, jnp.where(group == 0, a, b), jnp.where(group == 2, c, d)
        )
        crossed = jnp.where(
            group < 2, jnp.where(group == 0, b, a), jnp.where(group == 2, d, c)
        )
        crossed = jnp.where(even, pltpu.roll(crossed, 96, 1), pltpu.roll(crossed, 32, 1))
        rows = pl.ds(pl.multiple_of(beam * 16, 16), 16)
        field_re[rows, :] = jnp.where(even, straight, crossed)
        field_im[rows, :] = jnp.where(even, crossed, straight)

    def some_beams(step, carry):
        for inner in range(UNROLL):
            one_beam(step * UNROLL + inner)
        return carry

    lax.fori_loop(0, 128 // UNROLL, some_beams, 0)
    stores = []
    for piece in range(16):
        rows = pl.ds(piece, 128, stride=16)
        field = jnp.concatenate([field_re[rows, :], field_im[rows, :]], axis=1)
        field = field.astype(jnp.bfloat16)
        product = jnp.dot(coefficient[...], field, preferred_element_type=jnp.float32)
        real = product[:128, :128] - product[128:, 128:]
        imag = product[:128, 128:] + product[128:, :128]
        result[:, 128 * piece : 128 * piece + 128] = real * real + imag * imag
        if piece % 2 == 1:
            lanes = pl.ds(128 * (piece - 1), 256)
            store = pltpu.make_async_copy(
                result.at[:, lanes], out.at[:, lanes], beam_sem.at[1 + piece // 2]
            )
            store.start()
            stores.append(store)
    for store in stores:
        store.wait()


def body(
    atom_y, atom_x, atom_weight, beam_ky, beam_kx, beam_amplitude, crop_offset, probe_y, probe_x
):
    across, down, spread_y, spread_x = (jnp.asarray(v) for v in tables())
    vmem = pl.BlockSpec(memory_space=pltpu.VMEM)
    hbm = pl.BlockSpec(memory_space=pltpu.HBM)
    bf16 = jnp.bfloat16
    stay = functools.partial(pltpu.with_memory_space_constraint, memory_space=pltpu.HBM)
    core, coefficient, spread_y, spread_x, beams = pl.pallas_call(
        potential_kernel,
        name="potential_to_basis",
        out_shape=[
            jax.ShapeDtypeStruct((2, 192, 256), bf16),
            jax.ShapeDtypeStruct((256, 128), bf16),
            jax.ShapeDtypeStruct(spread_y.shape, bf16),
            jax.ShapeDtypeStruct(spread_x.shape, bf16),
            jax.ShapeDtypeStruct((4, 1, 128), jnp.int32),
        ],
        in_specs=[hbm] * 13,
        out_specs=[vmem] * 5,
        scratch_shapes=[
            pltpu.SMEM((2,), jnp.int32),
            pltpu.VMEM((3, 32, 128), jnp.float32),
            pltpu.VMEM((1, 128), jnp.float32),
            pltpu.VMEM((128 * GROUPS, N), bf16),
            pltpu.VMEM((BAND_ROWS, 128 * GROUPS), bf16),
            pltpu.VMEM((CHUNKS, COLS, 16, SLICE_WIDE), bf16),
            pltpu.VMEM((CHUNKS, COLS, 16, SLICE_WIDE), bf16),
            pltpu.VMEM((CHUNKS, COLS, 16, SLICE_WIDE), bf16),
            pltpu.VMEM((2 * CHUNK_ROWS, N), bf16),
            pltpu.VMEM((N, 512), bf16),
            pltpu.VMEM((2, 768, ROWS * TILE_Y), bf16),
            pltpu.VMEM((CHUNKS, CHUNK_ROWS, 256), bf16),
            pltpu.VMEM((CHUNKS, ROWS, CHUNK_ROWS, 256), bf16),
            pltpu.SemaphoreType.DMA((13,)),
            pltpu.SemaphoreType.DMA((CHUNKS, COLS)),
            pltpu.SemaphoreType.DMA((CHUNKS, COLS)),
            pltpu.SemaphoreType.DMA((CHUNKS, COLS)),
            pltpu.SemaphoreType.DMA((CHUNKS, COLS)),
            pltpu.SemaphoreType.DMA((CHUNKS, ROWS)),
            pltpu.SemaphoreType.DMA((CHUNKS, ROWS)),
        ],
        compiler_params=pltpu.CompilerParams(
            collective_id=0, has_side_effects=True, vmem_limit_bytes=24 * 2**20
        ),
    )(
        stay(crop_offset),
        stay(atom_y.reshape(32, 128)),
        stay(atom_x.reshape(32, 128)),
        stay(atom_weight.reshape(32, 128)),
        stay(beam_ky.reshape(1, 128)),
        stay(beam_kx.reshape(1, 128)),
        stay(beam_amplitude.reshape(1, 128)),
        stay(probe_y.reshape(1, 128)),
        stay(probe_x.reshape(1, 128)),
        stay(across),
        stay(down),
        stay(spread_y),
        stay(spread_x),
    )
    result = pl.pallas_call(
        probe_kernel,
        name="basis_to_probes",
        out_shape=jax.ShapeDtypeStruct((128, 2048), jnp.float32),
        in_specs=[vmem] * 5,
        out_specs=hbm,
        scratch_shapes=[
            pltpu.SMEM((2, 1, 128), jnp.int32),
            pltpu.VMEM((2, KINDS * TILE_Y, 128), bf16),
            pltpu.VMEM((128 * 16, 128), jnp.float32),
            pltpu.VMEM((128 * 16, 128), jnp.float32),
            pltpu.VMEM((128, 2048), jnp.float32),
            pltpu.SemaphoreType.DMA((9,)),
        ],
        compiler_params=pltpu.CompilerParams(vmem_limit_bytes=24 * 2**20),
    )(beams, core, coefficient, spread_y, spread_x)
    return result[None, None]


def solution(mesh):
    return jax.shard_map(
        body,
        mesh=mesh,
        in_specs=(
            P("col"),
            P("col"),
            P("col"),
            P(),
            P(),
            P(),
            P(),
            P("row", "col", None),
            P("row", "col", None),
        ),
        out_specs=P("row", "col", None, None),
        check_vma=False,
    )
```

```python
import functools
import math

import jax
import jax.numpy as jnp
import numpy as np
from jax import lax
from jax.experimental import pallas as pl
from jax.experimental.pallas import tpu as pltpu
from jax.sharding import PartitionSpec as P

N = 1024
WIN = 512
ROWS = 8
COLS = 16
TILT = 16
KINDS = 2 * TILT + 1
TILE_Y = WIN // ROWS
TILE_X = WIN // COLS
BAND_ROWS = N // ROWS
GROUPS = 7
CHUNKS = 2
UNROLL = 128
CHUNK_ROWS = BAND_ROWS // CHUNKS
SLICE_HIGH = CHUNK_ROWS // 16
SLICE_WIDE = N * SLICE_HIGH // COLS
LEAD = TILE_X * (COLS - 1)
MESH = pl.DeviceIdType.MESH


EDGE = np.concatenate([np.arange(N // 2 - TILT, N // 2), np.arange(-N // 2, -N // 2 + TILT)])
EDGES = (EDGE[EDGE % 2 != 0], EDGE[EDGE % 2 == 0])


def turn(number, modulus):
    return np.exp(2j * np.pi * np.mod(number, modulus) / modulus)


def fresnel():
    freq = np.arange(-N // 2, N // 2)
    half = np.arange(2 * N)
    return (turn(np.outer(half, freq), 2 * N) * turn(-freq * freq, 4 * N)[None, :]).sum(1) / N


def basis(length):
    table = fresnel()
    place = np.arange(N)
    shift = np.arange(length + TILT)
    rows = []
    for odd in (0, 1):
        apart = 2 * (shift[:, None] - TILT // 2 - place[None, :]) + odd
        edge = EDGES[odd]
        rows.append(table[np.mod(apart, 2 * N)])
        rows.append(turn(-edge * edge, 4 * N)[:, None] * turn(-np.outer(edge, place), N) / N)
    return np.concatenate(rows)


def synthesis(length):
    count = length + TILT
    pixel = np.arange(length)
    out = np.zeros((KINDS, length, count + TILT), complex)
    for kind in range(KINDS):
        tilt = kind - TILT
        odd = tilt % 2
        phase = turn(tilt * pixel, N)
        out[kind, pixel, pixel - (tilt + odd) // 2 + TILT // 2] = phase
        moved = EDGES[odd] + tilt
        flips = (moved < -N // 2) | (moved >= N // 2)
        wrapped = -2 * turn((2 * pixel[:, None] - tilt) * EDGES[odd][None, :], 2 * N)
        out[kind, :, count:] = phase[:, None] * np.where(flips[None, :], wrapped, 0)
    return out


def two_parts(value, axis):
    high = value.astype(jnp.bfloat16).astype(np.float64)
    return np.concatenate([high, value - high], axis)


@functools.lru_cache(None)
def tables():
    across = basis(TILE_X).T
    across = two_parts(np.concatenate([across.real, across.imag], 1), 1)
    across = np.concatenate([across[N - LEAD :], across], 0)
    down = basis(TILE_Y)
    down = two_parts(np.concatenate([down.real, down.imag], 0), 0)
    down = down.reshape(-1, ROWS, 2, TILE_Y).transpose(2, 0, 1, 3)
    down = down.reshape(2, down.shape[1], ROWS * TILE_Y)
    spread_y = synthesis(TILE_Y)
    order = (4 * np.arange(TILE_Y // 4)[None, :] + np.arange(4)[:, None]).reshape(-1)
    spread_y = np.concatenate([spread_y[0::2], spread_y[1::2]])[:, order]
    spread_y = np.concatenate([spread_y.real, spread_y.imag], 2).reshape(KINDS * TILE_Y, -1)
    spread_x = synthesis(TILE_X).transpose(0, 2, 1)
    top = np.concatenate([spread_x.real, spread_x.imag], 2)
    bottom = np.concatenate([-spread_x.imag, spread_x.real], 2)
    spread_x = np.concatenate([top, bottom], 1)
    spread_x = np.concatenate([spread_x, spread_x], 2)
    return tuple(
        value.astype(jnp.bfloat16) for value in (across, down, spread_y, spread_x)
    )


@functools.lru_cache(None)
def wave_fit():
    grid = np.cos(np.pi * (np.arange(4000) + 0.5) / 4000) * np.pi
    square = grid * grid
    powers = (square / np.pi**2)[:, None] ** np.arange(8)[None, :]
    even = np.linalg.lstsq(powers, np.cos(grid), rcond=None)[0] / np.pi ** (2 * np.arange(8))
    odd = np.linalg.lstsq(powers, np.sin(grid) / grid, rcond=None)[0] / np.pi ** (2 * np.arange(8))
    return [float(v) for v in even], [float(v) for v in odd]


def cos_sin_reduced(angle):
    even, odd = wave_fit()
    square = angle * angle
    cosine = jnp.full_like(angle, even[-1])
    sine = jnp.full_like(angle, odd[-1])
    for e, o in zip(even[-2::-1], odd[-2::-1]):
        cosine = cosine * square + e
        sine = sine * square + o
    return cosine, sine * angle


TURN_A = 6.28125
TURN_B = 0.0019350051879882812
TURN_C = 2.0 * math.pi - TURN_A - TURN_B


def cos_sin(angle):
    whole = jnp.floor(angle * (0.5 / math.pi) + 0.5)
    return cos_sin_reduced(((angle - whole * TURN_A) - whole * TURN_B) - whole * TURN_C)


def slice_place(block):
    high, side = block % SLICE_HIGH, block // SLICE_HIGH
    return (
        slice(16 * high, 16 * high + 16),
        slice(SLICE_WIDE * side, SLICE_WIDE * side + SLICE_WIDE),
    )


def potential_kernel(
    crop_hbm,
    atom_y_hbm,
    atom_x_hbm,
    atom_weight_hbm,
    tilt_y_hbm,
    tilt_x_hbm,
    amplitude_hbm,
    probe_y_hbm,
    probe_x_hbm,
    across_hbm,
    down_hbm,
    spread_y_hbm,
    spread_x_hbm,
    core,
    coefficient,
    spread_y,
    spread_x,
    beams,
    crop,
    atoms,
    amplitude,
    prof_x,
    prof_y,
    part,
    landed,
    whole,
    wave,
    across,
    down,
    moved,
    gathered,
    table_sem,
    part_send,
    part_recv,
    whole_send,
    whole_recv,
    moved_send,
    moved_recv,
):
    row = lax.axis_index("row")
    col = lax.axis_index("col")
    start = pl.multiple_of(LEAD - TILE_X * col, TILE_X)
    loads = [
        pltpu.make_async_copy(source, target, table_sem.at[place])
        for place, (source, target) in enumerate(
            (
                (crop_hbm, crop),
                (atom_y_hbm, atoms.at[0]),
                (atom_x_hbm, atoms.at[1]),
                (atom_weight_hbm, atoms.at[2]),
                (tilt_y_hbm, beams.at[0]),
                (tilt_x_hbm, beams.at[1]),
                (probe_y_hbm, beams.at[2]),
                (probe_x_hbm, beams.at[3]),
                (amplitude_hbm, amplitude),
                (across_hbm.at[pl.ds(start, N)], across),
                (down_hbm, down),
                (spread_y_hbm, spread_y),
                (spread_x_hbm, spread_x),
            )
        )
    ]
    for load in loads[:4]:
        load.start()
    barrier = pltpu.get_barrier_semaphore()
    for step in range(1, COLS):
        peer = lax.rem(col + step, COLS)
        pl.semaphore_signal(barrier, inc=1, device_id={"col": peer}, device_id_type=MESH)
    for step in range(1, ROWS):
        peer = lax.rem(row + step, ROWS)
        pl.semaphore_signal(barrier, inc=1, device_id={"row": peer}, device_id_type=MESH)
    for load in loads[4:9]:
        load.start()
    for load in loads[:4]:
        load.wait()

    crop_y = crop[0]
    crop_x = crop[1]
    first_y = (BAND_ROWS * row + crop_y) & (N - 1)
    first_group = ((first_y + (N - 21)) & (N - 1)) // 32
    at_y = ((lax.broadcasted_iota(jnp.int32, (BAND_ROWS, 128), 0) + first_y) & (N - 1)).astype(
        jnp.float32
    )
    lane = lax.broadcasted_iota(jnp.int32, (128, N), 1)
    at_x = ((lane + crop_x) & (N - 1)).astype(jnp.float32)
    for group in range(GROUPS):
        index = (first_group + group) & 31
        here_y = atoms[0, pl.ds(index, 1), :]
        here_x = atoms[1, pl.ds(index, 1), :]
        here_w = atoms[2, pl.ds(index, 1), :]
        apart = (at_y - here_y) * 0.5
        value = jnp.exp(-(apart * apart)) * here_w
        prof_y[:, 128 * group : 128 * group + 128] = value.astype(jnp.bfloat16)
        column = jnp.transpose(jnp.broadcast_to(here_x, (128, 128)))
        column = jnp.concatenate([column] * (N // 128), axis=1)
        apart = (at_x - column) * 0.5
        prof_x[128 * group : 128 * group + 128, :] = jnp.exp(-(apart * apart)).astype(jnp.bfloat16)
    partial = jnp.dot(prof_y[...], prof_x[...], preferred_element_type=jnp.float32)
    for chunk in range(CHUNKS):
        rows = partial[CHUNK_ROWS * chunk : CHUNK_ROWS * chunk + CHUNK_ROWS].astype(jnp.bfloat16)
        for block in range(COLS):
            part[chunk, block] = rows[slice_place(block)]
    pl.semaphore_wait(barrier, COLS - 1 + ROWS - 1)

    copies = []
    for chunk in range(CHUNKS):
        for step in range(1, COLS):
            peer = lax.rem(col + (COLS - step), COLS)
            copy = pltpu.make_async_remote_copy(
                src_ref=part.at[chunk, peer],
                dst_ref=landed.at[chunk, step],
                send_sem=part_send.at[chunk, step],
                recv_sem=part_recv.at[chunk, step],
                device_id={"col": peer},
                device_id_type=MESH,
            )
            copy.start()
            copies.append(copy)

    for load in loads[9:]:
        load.start()

    for load in loads[4:9]:
        load.wait()
    ky = beams[0]
    kx = beams[1]
    at_y = jnp.transpose(jnp.broadcast_to(beams[2], (128, 128))) - TILE_Y * row
    at_x = jnp.transpose(jnp.broadcast_to(beams[3], (128, 128))) - TILE_X * col
    number = (4 * (ky * at_y + kx * at_x) + ky * ky + kx * kx) & (4 * N - 1)
    number = jnp.where(number >= 2 * N, number - 4 * N, number)
    real, imag = cos_sin_reduced(number.astype(jnp.float32) * (-2.0 * math.pi / (4 * N)))
    weight = amplitude[...] * (1.0 / math.sqrt(128.0))
    coefficient[:128] = (real * weight).astype(jnp.bfloat16)
    coefficient[128:] = (imag * weight).astype(jnp.bfloat16)

    shares = []
    for chunk in range(CHUNKS):
        total = part[chunk, col].astype(jnp.float32)
        for step in range(1, COLS):
            copies[(COLS - 1) * chunk + step - 1].wait_recv()
            total = total + landed[chunk, step].astype(jnp.float32)
        whole[chunk, col] = (total - 1.0).astype(jnp.bfloat16)
        for step in range(1, COLS):
            peer = lax.rem(col + (COLS - step), COLS)
            share = pltpu.make_async_remote_copy(
                src_ref=whole.at[chunk, col],
                dst_ref=whole.at[chunk, col],
                send_sem=whole_send.at[chunk, step],
                recv_sem=whole_recv.at[chunk, step],
                device_id={"col": peer},
                device_id_type=MESH,
            )
            share.start()
            shares.append(share)

    loads[9].wait()
    hops = []
    for chunk in range(CHUNKS):
        for share in shares[(COLS - 1) * chunk : (COLS - 1) * (chunk + 1)]:
            share.wait_recv()
        for block in range(COLS):
            rows, columns = slice_place(block)
            real, imag = cos_sin(whole[chunk, block].astype(jnp.float32) + 1.0)
            wave[rows, columns] = real.astype(jnp.bfloat16)
            wave[slice(CHUNK_ROWS + rows.start, CHUNK_ROWS + rows.stop), columns] = imag.astype(
                jnp.bfloat16
            )
        product = jnp.dot(wave[...], across[...], preferred_element_type=jnp.float32)
        product = product[:, :256] + product[:, 256:]
        real = product[:CHUNK_ROWS, :128] - product[CHUNK_ROWS:, 128:]
        imag = product[:CHUNK_ROWS, 128:] + product[CHUNK_ROWS:, :128]
        both = jnp.concatenate([real, imag], axis=1).astype(jnp.bfloat16)
        moved[chunk] = both
        for step in range(1, ROWS):
            peer = lax.rem(row + step, ROWS)
            hop = pltpu.make_async_remote_copy(
                src_ref=moved.at[chunk],
                dst_ref=gathered.at[chunk, ((2 * row + chunk - peer + 16) & 15) // 2],
                send_sem=moved_send.at[chunk, step],
                recv_sem=moved_recv.at[chunk, step],
                device_id={"row": peer},
                device_id_type=MESH,
            )
            hop.start()
            hops.append(hop)
        gathered[chunk, ((row + chunk) & 15) // 2] = both

    loads[10].wait()
    product = None
    for chunk in range(CHUNKS):
        for hop in hops[(ROWS - 1) * chunk : (ROWS - 1) * (chunk + 1)]:
            hop.wait_recv()
        term = jnp.dot(
            down[(row + chunk) & 1],
            gathered[chunk].reshape(ROWS * TILE_Y, 256),
            preferred_element_type=jnp.float32,
        )
        product = term if product is None else product + term
    deep = product.shape[0] // 4
    product = product[: 2 * deep] + product[2 * deep :]
    real = product[:deep, :128] - product[deep:, 128:]
    imag = product[:deep, 128:] + product[deep:, :128]
    lower = lax.broadcasted_iota(jnp.int32, (deep, 128), 1) < 64
    real_turned = pltpu.roll(real, 64, 1)
    imag_turned = pltpu.roll(imag, 64, 1)
    rows = deep // 2
    for side, (first, second) in enumerate(
        (
            (jnp.where(lower, real, imag_turned), jnp.where(lower, -imag, real_turned)),
            (jnp.where(lower, real_turned, imag), jnp.where(lower, -imag_turned, real)),
        )
    ):
        for odd in (0, 1):
            mine = slice(rows * odd, rows * odd + rows)
            lanes = slice(128 * side, 128 * side + 128)
            core[odd, :rows, lanes] = first[mine].astype(jnp.bfloat16)
            core[odd, rows:, lanes] = second[mine].astype(jnp.bfloat16)
    for load in loads[11:]:
        load.wait()
    for copy in copies + shares + hops:
        copy.wait_send()


def probe_kernel(
    beams,
    core,
    coefficient,
    spread_y,
    spread_x,
    out,
    tilts,
    half,
    field_re,
    field_im,
    result,
    beam_sem,
):
    load = pltpu.make_async_copy(beams.at[pl.ds(0, 2)], tilts, beam_sem.at[0])
    load.start()

    middle = (KINDS // 2 + 1) * TILE_Y
    for odd, rows in enumerate((slice(0, middle), slice(middle, KINDS * TILE_Y))):
        value = jnp.dot(spread_y[rows], core[odd], preferred_element_type=jnp.float32)
        value = value.astype(jnp.bfloat16)
        half[0, rows] = value[:, :128]
        half[1, rows] = value[:, 128:]

    load.wait()
    group = lax.broadcasted_iota(jnp.int32, (16, 128), 1) // 32
    even = (group & 1) == 0

    def one_beam(beam):
        tilt = tilts[0, 0, beam]
        other = tilts[1, 0, beam]
        kind = (tilt & 1) * (KINDS // 2 + 1) + (tilt + TILT) // 2
        rows = pl.ds(pl.multiple_of(kind * TILE_Y, TILE_Y), TILE_Y)
        value = jnp.dot(
            half[other & 1, rows, :], spread_x[other + TILT], preferred_element_type=jnp.float32
        )
        a, b, c, d = (value[16 * i : 16 * i + 16] for i in range(4))
        straight = jnp.where(
            group < 2, jnp.where(group == 0, a, b), jnp.where(group == 2, c, d)
        )
        crossed = jnp.where(
            group < 2, jnp.where(group == 0, b, a), jnp.where(group == 2, d, c)
        )
        crossed = jnp.where(even, pltpu.roll(crossed, 96, 1), pltpu.roll(crossed, 32, 1))
        rows = pl.ds(pl.multiple_of(beam * 16, 16), 16)
        field_re[rows, :] = jnp.where(even, straight, crossed)
        field_im[rows, :] = jnp.where(even, crossed, straight)

    def some_beams(step, carry):
        for inner in range(UNROLL):
            one_beam(step * UNROLL + inner)
        return carry

    lax.fori_loop(0, 128 // UNROLL, some_beams, 0)
    stores = []
    for piece in range(16):
        rows = pl.ds(piece, 128, stride=16)
        field = jnp.concatenate([field_re[rows, :], field_im[rows, :]], axis=1)
        field = field.astype(jnp.bfloat16)
        product = jnp.dot(coefficient[...], field, preferred_element_type=jnp.float32)
        real = product[:128, :128] - product[128:, 128:]
        imag = product[:128, 128:] + product[128:, :128]
        result[:, 128 * piece : 128 * piece + 128] = real * real + imag * imag
        if piece % 2 == 1:
            lanes = pl.ds(128 * (piece - 1), 256)
            store = pltpu.make_async_copy(
                result.at[:, lanes], out.at[:, lanes], beam_sem.at[1 + piece // 2]
            )
            store.start()
            stores.append(store)
    for store in stores:
        store.wait()


def body(
    atom_y, atom_x, atom_weight, beam_ky, beam_kx, beam_amplitude, crop_offset, probe_y, probe_x
):
    across, down, spread_y, spread_x = (jnp.asarray(v) for v in tables())
    vmem = pl.BlockSpec(memory_space=pltpu.VMEM)
    hbm = pl.BlockSpec(memory_space=pltpu.HBM)
    bf16 = jnp.bfloat16
    stay = functools.partial(pltpu.with_memory_space_constraint, memory_space=pltpu.HBM)
    core, coefficient, spread_y, spread_x, beams = pl.pallas_call(
        potential_kernel,
        name="potential_to_basis",
        out_shape=[
            jax.ShapeDtypeStruct((2, 192, 256), bf16),
            jax.ShapeDtypeStruct((256, 128), bf16),
            jax.ShapeDtypeStruct(spread_y.shape, bf16),
            jax.ShapeDtypeStruct(spread_x.shape, bf16),
            jax.ShapeDtypeStruct((4, 1, 128), jnp.int32),
        ],
        in_specs=[hbm] * 13,
        out_specs=[vmem] * 5,
        scratch_shapes=[
            pltpu.SMEM((2,), jnp.int32),
            pltpu.VMEM((3, 32, 128), jnp.float32),
            pltpu.VMEM((1, 128), jnp.float32),
            pltpu.VMEM((128 * GROUPS, N), bf16),
            pltpu.VMEM((BAND_ROWS, 128 * GROUPS), bf16),
            pltpu.VMEM((CHUNKS, COLS, 16, SLICE_WIDE), bf16),
            pltpu.VMEM((CHUNKS, COLS, 16, SLICE_WIDE), bf16),
            pltpu.VMEM((CHUNKS, COLS, 16, SLICE_WIDE), bf16),
            pltpu.VMEM((2 * CHUNK_ROWS, N), bf16),
            pltpu.VMEM((N, 512), bf16),
            pltpu.VMEM((2, 768, ROWS * TILE_Y), bf16),
            pltpu.VMEM((CHUNKS, CHUNK_ROWS, 256), bf16),
            pltpu.VMEM((CHUNKS, ROWS, CHUNK_ROWS, 256), bf16),
            pltpu.SemaphoreType.DMA((13,)),
            pltpu.SemaphoreType.DMA((CHUNKS, COLS)),
            pltpu.SemaphoreType.DMA((CHUNKS, COLS)),
            pltpu.SemaphoreType.DMA((CHUNKS, COLS)),
            pltpu.SemaphoreType.DMA((CHUNKS, COLS)),
            pltpu.SemaphoreType.DMA((CHUNKS, ROWS)),
            pltpu.SemaphoreType.DMA((CHUNKS, ROWS)),
        ],
        compiler_params=pltpu.CompilerParams(
            collective_id=0, has_side_effects=True, vmem_limit_bytes=24 * 2**20
        ),
    )(
        stay(crop_offset),
        stay(atom_y.reshape(32, 128)),
        stay(atom_x.reshape(32, 128)),
        stay(atom_weight.reshape(32, 128)),
        stay(beam_ky.reshape(1, 128)),
        stay(beam_kx.reshape(1, 128)),
        stay(beam_amplitude.reshape(1, 128)),
        stay(probe_y.reshape(1, 128)),
        stay(probe_x.reshape(1, 128)),
        stay(across),
        stay(down),
        stay(spread_y),
        stay(spread_x),
    )
    result = pl.pallas_call(
        probe_kernel,
        name="basis_to_probes",
        out_shape=jax.ShapeDtypeStruct((128, 2048), jnp.float32),
        in_specs=[vmem] * 5,
        out_specs=hbm,
        scratch_shapes=[
            pltpu.SMEM((2, 1, 128), jnp.int32),
            pltpu.VMEM((2, KINDS * TILE_Y, 128), bf16),
            pltpu.VMEM((128 * 16, 128), jnp.float32),
            pltpu.VMEM((128 * 16, 128), jnp.float32),
            pltpu.VMEM((128, 2048), jnp.float32),
            pltpu.SemaphoreType.DMA((9,)),
        ],
        compiler_params=pltpu.CompilerParams(vmem_limit_bytes=24 * 2**20),
    )(beams, core, coefficient, spread_y, spread_x)
    return result[None, None]


def solution(mesh):
    return jax.shard_map(
        body,
        mesh=mesh,
        in_specs=(
            P("col"),
            P("col"),
            P("col"),
            P(),
            P(),
            P(),
            P(),
            P("row", "col", None),
            P("row", "col", None),
        ),
        out_specs=P("row", "col", None, None),
        check_vma=False,
    )
```
